32 devices in a mesh: sub: 4 (over x, core), gx: 4 (over z), gy: 2 (over y).
Axes of the slice: x: 2, y: 2, z: 4, core: 2. Of those that a mesh axis runs over, the one named last changes fastest.
Arguments:
- state: float32 [4, 256, 512], P(None, ('sub', 'gx'), 'gy'), may hold values from -4 to 4
- damping: float32 [4, 256, 512], P(None, ('sub', 'gx'), 'gy'), may hold values from 0.005 to 0.1
- weights: float32 [4], replicated, may hold values from 0.5 to 1.5
Outputs:
- combined: float32 [4, 256, 512], P(None, ('sub', 'gx'), 'gy')
- column_error: float32 [4, 512], P(None, 'gy')
The draws below stay inside these ranges and needn't reach their ends.
All inputs are finite; a program needn't handle non-finite values.
Results may differ from the reference program's by a relative error of at most 0.0003.
Values sent between devices are 32-bit elements; how exact they have to be, the bound alone decides.
No kernel may reach another device: no remote copies, remote signals or barrier semaphores. Data moves between devices by JAX's collectives and lax.ppermute only.
A program may use at most 64 MiB of HBM per device.

```python
import math
import jax
import jax.numpy as jnp
from jax import lax

FIELDS = 4
KRYLOV = 12
SUBSTEPS = 4
NX = 256
NY = 512


def block_scale(stream_key, dims, shards, smallest, top_value):
    factor_of = 1.0
    for dim, parts in shards:
        draws = jax.random.uniform(jax.random.fold_in(jax.random.fold_in(stream_key, 6), dim), (parts,), jnp.float32, smallest / len(shards), top_value / len(shards))
        factor_of = factor_of * jnp.repeat(jnp.exp(draws), dims[dim] // parts).reshape((-1,) + (1,) * (len(dims) - 1 - dim))
    return factor_of


def scatter_about(stream_key, shape, width, limit, pieces=(), kind=jnp.bfloat16):
    entries = jax.random.normal(stream_key, shape, jnp.float32) * width
    if len(pieces) > 0:
        entries = block_scale(stream_key, shape, pieces, -0.22, 0.18) * entries
    return jnp.clip(entries, min=-limit, max=limit).astype(kind)


def setup_inputs(seed: int = 0) -> dict:
    key_list = jax.random.split(jax.random.key(seed), 4)
    return {
        "state": scatter_about(key_list[0], (FIELDS, NX, NY), 1.0, 4.0, ((1, 16), (2, 2)), jnp.float32),
        "damping": jnp.clip(jnp.exp(math.log(0.1) - 2.9957323 * jax.random.uniform(key_list[1], (FIELDS, NX, NY), jnp.float32) ** block_scale(key_list[1], (FIELDS, NX, NY), ((1, 16), (2, 2)), -0.2, 0.2)), 0.005, 0.1),
        "weights": jnp.clip(jax.random.uniform(key_list[2], (SUBSTEPS,), jnp.float32, 0.5, 1.5), 0.5, 1.5),
    }


dt_total = 4.0
sound_sq = 1.0
buoyancy_sq = 0.5
norm_eps = 1e-06
taylor_degree = 12
squarings = 8

def tendencies(padded):
    velocity_x = padded[0]
    velocity_y = padded[1]
    buoyancy = padded[2]
    pressure = padded[3]
    rise_x = 0.5 * (pressure[2:, 1:-1] - pressure[:-2, 1:-1])
    rise_y = 0.5 * (pressure[1:-1, 2:] - pressure[1:-1, :-2])
    spread = 0.5 * (velocity_x[2:, 1:-1] - velocity_x[:-2, 1:-1]) + 0.5 * (velocity_y[1:-1, 2:] - velocity_y[1:-1, :-2])
    return jnp.stack([-rise_x, -rise_y + buoyancy[1:-1, 1:-1], -buoyancy_sq * velocity_y[1:-1, 1:-1], -sound_sq * spread])

def wave(field):
    return tendencies(jnp.pad(field, ((0, 0), (1, 1), (1, 1))))

def phi_first(hessenberg):
    extent = hessenberg.shape[0]
    augmented = jnp.zeros((extent + 1, extent + 1), jnp.float32)
    augmented = augmented.at[:extent, :extent].set(hessenberg).at[0, extent].set(1.0)
    scaled = augmented / 2.0 ** squarings
    result = jnp.eye(extent + 1, dtype=jnp.float32)
    power_term = result
    for degree in range(1, taylor_degree + 1):
        power_term = jnp.dot(power_term, scaled, precision=lax.Precision.HIGHEST) / degree
        result = result + power_term
    for repeat in range(squarings):
        result = jnp.dot(result, result, precision=lax.Precision.HIGHEST)
    return result[:extent, extent]

def reference(state, damping, weights):
    stiffness = 3.0 * damping * state * state
    forcing = wave(state) - damping * state * state * state
    beta_norm = jnp.sqrt(jnp.sum(forcing * forcing) + norm_eps)
    vectors = [forcing / beta_norm]
    hessenberg = jnp.zeros((KRYLOV + 1, KRYLOV), jnp.float32)
    for column in range(KRYLOV):
        current = vectors[column]
        image = dt_total * (wave(current) - stiffness * current)
        products = jnp.stack([jnp.sum(vector * image) for vector in vectors])
        for index_row in range(column + 1):
            image = image - products[index_row] * vectors[index_row]
        length = jnp.sqrt(jnp.sum(image * image) + norm_eps)
        hessenberg = hessenberg.at[:column + 1, column].set(products).at[column + 1, column].set(length)
        vectors.append(image / length)
    mixing = jnp.zeros((KRYLOV,), jnp.float32)
    highest = jnp.zeros((), jnp.float32)
    for member in range(SUBSTEPS):
        fraction = (member + 1) / SUBSTEPS
        factor = dt_total * fraction
        coefficients = phi_first(fraction * hessenberg[:KRYLOV])
        mixing = mixing + weights[member] * factor * beta_norm * coefficients
        estimate = factor * beta_norm * fraction * hessenberg[KRYLOV, KRYLOV - 1] * jnp.abs(coefficients[KRYLOV - 1])
        highest = jnp.maximum(highest, estimate)
    combined = state
    for index_row in range(KRYLOV):
        combined = combined + mixing[index_row] * vectors[index_row]
    column_error = highest * lax.optimization_barrier(jnp.max(jnp.abs(vectors[KRYLOV]), axis=1))
    return (combined, column_error)
```

```python
import functools

import jax
import jax.numpy as jnp
from jax import lax
from jax.experimental import pallas as pl
from jax.experimental.pallas import tpu as pltpu
from jax.sharding import PartitionSpec as P

KRYLOV = 12
SUBSTEPS = 4
STEPS = 4
HALO = 16
LANES = 128
SLOTS = 16

dt_total = 4.0
buoyancy_sq = 0.5
norm_eps = 1e-06
taylor_degree = 12
squarings = 8
SHIFT = -2.0
RADIUS = 4.0

ROWS = ("sub", "gx")
ALL = ("sub", "gx", "gy")
HIGH = lax.Precision.HIGHEST
VMEM = pl.BlockSpec(memory_space=pltpu.VMEM)


def iota(shape, dim):
    return lax.broadcasted_iota(jnp.int32, shape, dim)


def rise_rows(x):
    return pltpu.roll(x, x.shape[0] - 1, 0) - pltpu.roll(x, 1, 0)


def rise_columns(x):
    return pltpu.roll(x, x.shape[1] - 1, 1) - pltpu.roll(x, 1, 1)


def grid_mask(rows, columns, halo_rows):
    line, lane = iota((rows, columns), 0), iota((rows, columns), 1)
    place = lax.axis_index("sub") * lax.axis_size("gx") + lax.axis_index("gx")
    last = lax.axis_size("sub") * lax.axis_size("gx") - 1
    side = lax.axis_index("gy")
    first_line = jnp.where(place > 0, 0, halo_rows)
    end_line = jnp.where(place < last, rows, rows - halo_rows)
    body = columns - LANES
    right_end = jnp.where(side < lax.axis_size("gy") - 1, body + LANES // 2, body)
    left_start = jnp.where(side > 0, body + LANES // 2, columns)
    inside = (line >= first_line) & (line < end_line) & ((lane < right_end) | (lane >= left_start))
    return jnp.where(inside, 1.0, 0.0)


def power_step(fields, drag, half):
    vx, vy, b, p = fields
    quarter = dt_total / RADIUS
    return (
        -half * rise_rows(p) - drag[0] * vx,
        -half * rise_columns(p) + quarter * b - drag[1] * vy,
        (-buoyancy_sq * quarter) * vy - drag[2] * b,
        -half * (rise_rows(vx) + rise_columns(vy)) - drag[3] * p,
    )


def pair_rows(one, two):
    total = None
    for f in range(4):
        prod = one[f] * two[f]
        part = None
        for r in range(0, prod.shape[0], 8):
            for c in range(0, prod.shape[1], LANES):
                tile = prod[r : r + 8, c : c + LANES]
                part = tile if part is None else part + tile
        total = part if total is None else total + part
    return jnp.sum(total, axis=0, keepdims=True)


def gram_out(old, new, table_ref, send_ref):
    first = len(old)
    table_ref[...] = jnp.zeros_like(table_ref)
    for j in range(len(new)):
        for i in range(first):
            table_ref[j * SLOTS + i : j * SLOTS + i + 1, :] = pair_rows(old[i](), new[j]())
        for i in range(j + 1):
            row = pair_rows(new[i](), new[j]())
            table_ref[j * SLOTS + first + i : j * SLOTS + first + i + 1, :] = row
            if i != j:
                table_ref[i * SLOTS + first + j : i * SLOTS + first + j + 1, :] = row
    packed = lax.dot_general(
        jnp.ones((8, LANES), jnp.float32),
        table_ref[...],
        (((1,), (1,)), ((), ())),
        precision=HIGH,
        preferred_element_type=jnp.float32,
    )
    for d in range(send_ref.shape[0]):
        send_ref[d] = packed[0:1]


def first_kernel(own_ref, up_ref, down_ref, basis_ref, drag_ref, send_ref, table_ref):
    rows = own_ref.shape[2] + 2 * HALO
    columns = own_ref.shape[3]
    mask = grid_mask(rows, columns, HALO)

    def whole(kind, f):
        joined = jnp.concatenate([up_ref[kind, f], own_ref[kind, f], down_ref[kind, f]], axis=0)
        return jnp.where(mask > 0, joined, 0.0)

    state = [whole(0, f) for f in range(4)]
    damping = [whole(1, f) for f in range(4)]
    vx, vy, b, p = state
    half = 0.5 * mask
    linear = (
        -half * rise_rows(p),
        -half * rise_columns(p) + b,
        -buoyancy_sq * vy,
        -half * (rise_rows(vx) + rise_columns(vy)),
    )
    for f in range(4):
        square = damping[f] * state[f] * state[f]
        basis_ref[0, f] = linear[f] - square * state[f]
        drag_ref[f] = (3.0 * dt_total / RADIUS) * square + SHIFT / RADIUS
    half = (0.5 * dt_total / RADIUS) * mask
    for step in range(STEPS):
        current = [basis_ref[step, f] for f in range(4)]
        drag = [drag_ref[f] for f in range(4)]
        for f, value in enumerate(power_step(current, drag, half)):
            basis_ref[step + 1, f] = value
    body = columns - LANES

    def interior(j):
        return lambda: [basis_ref[j, f, HALO : rows - HALO, :body] for f in range(4)]

    gram_out([], [interior(j) for j in range(STEPS + 1)], table_ref, send_ref)


def gram_matrix(received_ref, first):
    packed = jnp.sum(received_ref[...], axis=0)
    tile = (SLOTS, LANES)
    row, lane = iota(tile, 0), iota(tile, 1)
    tall = (LANES, LANES)
    tall_row, tall_lane = iota(tall, 0), iota(tall, 1)
    packed = jnp.broadcast_to(packed, tile)
    dot = functools.partial(jnp.dot, precision=HIGH, preferred_element_type=jnp.float32)
    by_row = jnp.where(lane % SLOTS == row, packed, 0.0)
    right = dot(by_row, jnp.where(tall_row // SLOTS == tall_lane - first, 1.0, 0.0))
    by_column = jnp.where(lane // SLOTS == row - first, packed, 0.0)
    below = dot(by_column, jnp.where(tall_row % SLOTS == tall_lane, 1.0, 0.0))
    unit = jnp.where(row == lane, 1.0, 0.0)
    return jnp.where(lane >= first, right, jnp.where(row >= first, below, unit)), unit


def orthogonalize(gram, unit, first, hess):
    tile = (SLOTS, LANES)
    row, lane = iota(tile, 0), iota(tile, 1)
    down = lambda x: jnp.sum(x, axis=0, keepdims=True)
    across = lambda x: jnp.sum(x, axis=1, keepdims=True)
    fresh = (row >= first) & (row < first + STEPS)
    chain = jnp.where(fresh & (lane == row), SHIFT, 0.0) + jnp.where(fresh & (lane == row + 1), RADIUS, 0.0)
    steps = hess + chain
    old = row < first
    beta = None
    if first == 0:
        beta = jnp.sqrt(gram[0:1, 0:1] + norm_eps)
        start = 1.0 / beta
    else:
        start = jnp.ones((1, 1), jnp.float32)
    scale = jnp.where(row == first, start, jnp.where(old, 1.0, 0.0))
    coefs = unit * scale
    images = gram * scale
    column = jnp.where(row[:, 0:1] == first, start, 0.0)
    for c in range(first, first + STEPS):
        z = down(steps * column)
        products = across(images * z)
        z = z - down(coefs * products)
        column = across(unit * z)
        image = across(gram * z)
        length = jnp.sqrt(jnp.maximum(down(column * image), 0.0) + norm_eps)
        inverse = 1.0 / length
        hess_row = down(unit * products) + jnp.where(lane[0:1] == c + 1, length, 0.0)
        hess = jnp.where(row == c, hess_row, hess)
        coefs = jnp.where(row == c + 1, z * inverse, coefs)
        images = jnp.where(row == c + 1, down(gram * column) * inverse, images)
        column = column * inverse
    return coefs, hess, beta


def combine(coefs, c, parts):
    total = None
    for i, part in parts:
        term = coefs[c : c + 1, i : i + 1] * part()
        total = term if total is None else total + term
    return total


def next_kernel(first, received_ref, small_ref, drag_in_ref, old_ref, basis_in_ref, basis_ref, kept_ref, small_out_ref, send_ref, table_ref):
    edge = (basis_in_ref.shape[2] - basis_ref.shape[2]) // 2
    rows, columns = basis_ref.shape[2:]
    gram, unit = gram_matrix(received_ref, first)
    hess = small_ref[0] if first else jnp.zeros((SLOTS, LANES), jnp.float32)
    coefs, hess, beta = orthogonalize(gram, unit, first, hess)
    small_out_ref[0] = hess
    small_out_ref[1] = jnp.broadcast_to(beta, (SLOTS, LANES)) if first == 0 else small_ref[1]
    for f in range(4):
        parts = [(first + j, lambda j=j: basis_in_ref[j, f, edge : edge + rows]) for j in range(STEPS + 1)]
        if first:
            for i in range(first):
                kept_ref[i, f] = old_ref[i, f]
            parts = [(i, lambda i=i: old_ref[i, f]) for i in range(first)] + parts
        for c in range(first, first + STEPS):
            kept_ref[c, f] = combine(coefs, c, parts[: c + 1])
        basis_ref[0, f] = combine(coefs, first + STEPS, parts)
    halo = (rows - (drag_in_ref.shape[1] - 2 * HALO)) // 2
    half = (0.5 * dt_total / RADIUS) * grid_mask(rows, columns, halo)
    skip = HALO - halo
    for step in range(STEPS):
        current = [basis_ref[step, f] for f in range(4)]
        drag = [drag_in_ref[f, skip : skip + rows] for f in range(4)]
        for f, value in enumerate(power_step(current, drag, half)):
            basis_ref[step + 1, f] = value
    body = columns - LANES

    def interior(ref, j):
        return lambda: [ref[j, f, halo : rows - halo, :body] for f in range(4)]

    gram_out(
        [interior(kept_ref, i) for i in range(first + STEPS)],
        [interior(basis_ref, j) for j in range(STEPS + 1)],
        table_ref,
        send_ref,
    )


def last_kernel(first, received_ref, small_ref, old_ref, basis_ref, small_out_ref, peak_ref):
    rows, columns = basis_ref.shape[2:]
    body = columns - LANES
    halo = HALO // 2
    gram, unit = gram_matrix(received_ref, first)
    coefs, hess, _ = orthogonalize(gram, unit, first, small_ref[0])
    small_out_ref[0] = hess
    small_out_ref[1] = small_ref[1]
    small_out_ref[2] = coefs
    tiles = body // LANES
    for f in range(4):
        parts = [(i, lambda i=i: old_ref[i, f, halo : rows - halo, :body]) for i in range(first)]
        parts += [(first + j, lambda j=j: basis_ref[j, f, halo : rows - halo, :body]) for j in range(STEPS + 1)]
        peak = jnp.max(jnp.abs(combine(coefs, KRYLOV, parts)), axis=0, keepdims=True)
        for d in range(peak_ref.shape[0]):
            for t in range(tiles):
                peak_ref[d, f * tiles + t : f * tiles + t + 1, :] = peak[:, t * LANES : (t + 1) * LANES]


def finish_kernel(first, weights_ref, small_ref, state_ref, old_ref, basis_ref, peaks_ref, combined_ref, error_ref):
    rows, columns = basis_ref.shape[2:]
    body = columns - LANES
    halo = HALO // 2
    hess, beta, coefs = small_ref[0], small_ref[1, 0:1, 0:1], small_ref[2]
    dot = functools.partial(jnp.dot, precision=HIGH, preferred_element_type=jnp.float32)
    size = SUBSTEPS * SLOTS
    row, lane = iota((size, LANES), 0), iota((size, LANES), 1)
    row_in, lane_in = row % SLOTS, lane % SLOTS
    same = (row // SLOTS == lane // SLOTS) & (lane < size)
    spread = jnp.where(iota((LANES, LANES), 0) == iota((LANES, LANES), 1) % SLOTS, 1.0, 0.0)
    wide = dot(jnp.concatenate([hess] * SUBSTEPS, axis=0), spread)
    fraction = ((row // SLOTS) + 1).astype(jnp.float32) * (1.0 / SUBSTEPS)
    scaled = jnp.where(same & (row_in < KRYLOV) & (lane_in < KRYLOV), wide * fraction, 0.0)
    scaled = scaled + jnp.where(same & (row_in == KRYLOV) & (lane_in == 0), 1.0, 0.0)
    scaled = scaled * (1.0 / 2.0**squarings)
    unit = jnp.where(row == lane, 1.0, 0.0)
    pad = jnp.zeros((LANES - size, LANES), jnp.float32)

    def times(a, b):
        return dot(a, jnp.concatenate([b, pad], axis=0))

    result, term = unit, unit
    for degree in range(1, taylor_degree + 1):
        term = times(term, scaled) * (1.0 / degree)
        result = result + term
    for _ in range(squarings):
        result = times(result, result)
    mixing = jnp.zeros((1, LANES), jnp.float32)
    highest = jnp.zeros((1, 1), jnp.float32)
    gather = jnp.where(iota((LANES, LANES), 0) % SLOTS == iota((LANES, LANES), 1), 1.0, 0.0)
    for k in range(SUBSTEPS):
        tau = (k + 1) / SUBSTEPS
        factor = dt_total * tau
        g = result[k * SLOTS + KRYLOV : k * SLOTS + KRYLOV + 1, :]
        mixing = mixing + jnp.where(lane[0:1] // SLOTS == k, weights_ref[k] * factor, 0.0) * beta * g
        last = jnp.abs(g[:, k * SLOTS + KRYLOV - 1 : k * SLOTS + KRYLOV])
        estimate = (factor * tau) * beta * hess[KRYLOV - 1 : KRYLOV, KRYLOV : KRYLOV + 1] * last
        highest = jnp.maximum(highest, estimate)
    mixing = jnp.where(lane_in[0:1] < KRYLOV, mixing, 0.0)
    mixing = dot(jnp.broadcast_to(mixing, (8, LANES)), gather)
    coef_pad = jnp.concatenate([coefs, jnp.zeros((LANES - SLOTS, LANES), jnp.float32)], axis=0)
    share = dot(jnp.where(iota((8, LANES), 1) < KRYLOV, mixing, 0.0), coef_pad)
    for f in range(4):
        parts = [(i, lambda i=i: old_ref[i, f, halo : rows - halo, :body]) for i in range(first)]
        parts += [(first + j, lambda j=j: basis_ref[j, f, halo : rows - halo, :body]) for j in range(STEPS + 1)]
        combined_ref[f] = state_ref[f] + combine(share, 0, parts)
    peak = jnp.max(peaks_ref[...], axis=0) * highest
    tiles = body // LANES
    for f in range(4):
        for t in range(tiles):
            error_ref[f : f + 1, t * LANES : (t + 1) * LANES] = peak[f * tiles + t : f * tiles + t + 1]


def shards(state, damping, weights):
    fields, height, width = state.shape
    body = width
    columns = width + LANES
    devices = lax.axis_size("sub") * lax.axis_size("gx") * lax.axis_size("gy")
    lines = lax.axis_size("sub") * lax.axis_size("gx")
    sides = lax.axis_size("gy")
    f32 = functools.partial(jax.ShapeDtypeStruct, dtype=jnp.float32)
    pair = jnp.stack([state, damping])
    head, tail = pair[..., :LANES], pair[..., body - LANES :]
    if sides == 2:
        halo = lax.ppermute(jnp.where(lax.axis_index("gy") == 0, tail, head), "gy", [(0, 1), (1, 0)])
    else:
        from_right = lax.ppermute(head, "gy", [((i + 1) % sides, i) for i in range(sides)])
        from_left = lax.ppermute(tail, "gy", [(i, (i + 1) % sides) for i in range(sides)])
        halo = jnp.concatenate([from_right[..., : LANES // 2], from_left[..., LANES // 2 :]], axis=-1)
    own = jnp.concatenate([pair, halo], axis=-1)
    up = lax.ppermute(own[:, :, height - HALO :], ROWS, [(i, (i + 1) % lines) for i in range(lines)])
    down = lax.ppermute(own[:, :, :HALO], ROWS, [((i + 1) % lines, i) for i in range(lines)])

    def call(body_fn, outs, *args, smem=(), scratch=()):
        specs = [pl.BlockSpec(memory_space=pltpu.SMEM) if k in smem else VMEM for k in range(len(args))]
        return pl.pallas_call(
            body_fn,
            out_shape=outs,
            in_specs=specs,
            out_specs=[VMEM] * len(outs),
            scratch_shapes=list(scratch),
        )(*args)

    table = pltpu.VMEM((LANES, LANES), jnp.float32)
    send_shape = f32((devices, 1, LANES))
    small_shape = f32((2, SLOTS, LANES))
    tall = height + 2 * HALO
    short = height + HALO
    basis, drag, send = call(
        first_kernel,
        [f32((STEPS + 1, fields, tall, columns)), f32((fields, tall, columns)), send_shape],
        own,
        up,
        down,
        scratch=[table],
    )
    exchange = lambda x, axes: lax.all_to_all(x, axes, 0, 0)
    received = exchange(send, ALL)
    small = jnp.zeros((2, SLOTS, LANES), jnp.float32)
    kept = drag
    for first in range(0, KRYLOV - STEPS, STEPS):
        basis, kept, small, send = call(
            functools.partial(next_kernel, first),
            [
                f32((STEPS + 1, fields, short, columns)),
                f32((first + STEPS, fields, short, columns)),
                small_shape,
                send_shape,
            ],
            received,
            small,
            drag,
            kept,
            basis,
            scratch=[table],
        )
        received = exchange(send, ALL)
    first = KRYLOV - STEPS
    peak_rows = fields * (body // LANES)
    small, peaks = call(
        functools.partial(last_kernel, first),
        [f32((3, SLOTS, LANES)), f32((lines, peak_rows, LANES))],
        received,
        small,
        kept,
        basis,
    )
    peaks = exchange(peaks, ROWS)
    combined, column_error = call(
        functools.partial(finish_kernel, first),
        [f32((fields, height, width)), f32((fields, width))],
        weights,
        small,
        state,
        kept,
        basis,
        peaks,
        smem=(0,),
    )
    return combined, column_error


def solution(mesh):
    return jax.shard_map(
        shards,
        mesh=mesh,
        in_specs=(P(None, ROWS, "gy"), P(None, ROWS, "gy"), P()),
        out_specs=(P(None, ROWS, "gy"), P(None, "gy")),
        check_vma=False,
    )
```

```python
import functools

import jax
import jax.numpy as jnp
from jax import lax
from jax.experimental import pallas as pl
from jax.experimental.pallas import tpu as pltpu
from jax.sharding import PartitionSpec as P

KRYLOV = 12
SUBSTEPS = 4
STEPS = 4
HALO = 16
LANES = 128
SLOTS = 16

dt_total = 4.0
buoyancy_sq = 0.5
norm_eps = 1e-06
taylor_degree = 12
squarings = 8
SHIFT = -2.0
RADIUS = 4.0

ROWS = ("sub", "gx")
ALL = ("sub", "gx", "gy")
HIGH = lax.Precision.HIGHEST
VMEM = pl.BlockSpec(memory_space=pltpu.VMEM)


def iota(shape, dim):
    return lax.broadcasted_iota(jnp.int32, shape, dim)


def rise_rows(x):
    return pltpu.roll(x, x.shape[0] - 1, 0) - pltpu.roll(x, 1, 0)


def rise_columns(x):
    return pltpu.roll(x, x.shape[1] - 1, 1) - pltpu.roll(x, 1, 1)


def grid_mask(rows, columns, halo_rows):
    line, lane = iota((rows, columns), 0), iota((rows, columns), 1)
    place = lax.axis_index("sub") * lax.axis_size("gx") + lax.axis_index("gx")
    last = lax.axis_size("sub") * lax.axis_size("gx") - 1
    side = lax.axis_index("gy")
    first_line = jnp.where(place > 0, 0, halo_rows)
    end_line = jnp.where(place < last, rows, rows - halo_rows)
    body = columns - LANES
    right_end = jnp.where(side < lax.axis_size("gy") - 1, body + LANES // 2, body)
    left_start = jnp.where(side > 0, body + LANES // 2, columns)
    inside = (line >= first_line) & (line < end_line) & ((lane < right_end) | (lane >= left_start))
    return jnp.where(inside, 1.0, 0.0)


def power_step(fields, drag, half):
    vx, vy, b, p = fields
    quarter = dt_total / RADIUS
    return (
        -half * rise_rows(p) - drag[0] * vx,
        -half * rise_columns(p) + quarter * b - drag[1] * vy,
        (-buoyancy_sq * quarter) * vy - drag[2] * b,
        -half * (rise_rows(vx) + rise_columns(vy)) - drag[3] * p,
    )


def pair_rows(one, two):
    total = None
    for f in range(4):
        prod = one[f] * two[f]
        part = None
        for r in range(0, prod.shape[0], 8):
            for c in range(0, prod.shape[1], LANES):
                tile = prod[r : r + 8, c : c + LANES]
                part = tile if part is None else part + tile
        total = part if total is None else total + part
    return jnp.sum(total, axis=0, keepdims=True)


def gram_out(old, new, table_ref, send_ref):
    first = len(old)
    table_ref[...] = jnp.zeros_like(table_ref)
    for j in range(len(new)):
        for i in range(first):
            table_ref[j * SLOTS + i : j * SLOTS + i + 1, :] = pair_rows(old[i](), new[j]())
        for i in range(j + 1):
            row = pair_rows(new[i](), new[j]())
            table_ref[j * SLOTS + first + i : j * SLOTS + first + i + 1, :] = row
            if i != j:
                table_ref[i * SLOTS + first + j : i * SLOTS + first + j + 1, :] = row
    packed = lax.dot_general(
        jnp.ones((8, LANES), jnp.float32),
        table_ref[...],
        (((1,), (1,)), ((), ())),
        precision=HIGH,
        preferred_element_type=jnp.float32,
    )
    for d in range(send_ref.shape[0]):
        send_ref[d] = packed[0:1]


def first_kernel(own_ref, up_ref, down_ref, basis_ref, drag_ref, send_ref, table_ref):
    rows = own_ref.shape[2] + 2 * HALO
    columns = own_ref.shape[3]
    mask = grid_mask(rows, columns, HALO)

    def whole(kind, f):
        joined = jnp.concatenate([up_ref[kind, f], own_ref[kind, f], down_ref[kind, f]], axis=0)
        return jnp.where(mask > 0, joined, 0.0)

    state = [whole(0, f) for f in range(4)]
    damping = [whole(1, f) for f in range(4)]
    vx, vy, b, p = state
    half = 0.5 * mask
    linear = (
        -half * rise_rows(p),
        -half * rise_columns(p) + b,
        -buoyancy_sq * vy,
        -half * (rise_rows(vx) + rise_columns(vy)),
    )
    for f in range(4):
        square = damping[f] * state[f] * state[f]
        basis_ref[0, f] = linear[f] - square * state[f]
        drag_ref[f] = (3.0 * dt_total / RADIUS) * square + SHIFT / RADIUS
    half = (0.5 * dt_total / RADIUS) * mask
    for step in range(STEPS):
        current = [basis_ref[step, f] for f in range(4)]
        drag = [drag_ref[f] for f in range(4)]
        for f, value in enumerate(power_step(current, drag, half)):
            basis_ref[step + 1, f] = value
    body = columns - LANES

    def interior(j):
        return lambda: [basis_ref[j, f, HALO : rows - HALO, :body] for f in range(4)]

    gram_out([], [interior(j) for j in range(STEPS + 1)], table_ref, send_ref)


def gram_matrix(received_ref, first):
    packed = jnp.sum(received_ref[...], axis=0)
    tile = (SLOTS, LANES)
    row, lane = iota(tile, 0), iota(tile, 1)
    tall = (LANES, LANES)
    tall_row, tall_lane = iota(tall, 0), iota(tall, 1)
    packed = jnp.broadcast_to(packed, tile)
    dot = functools.partial(jnp.dot, precision=HIGH, preferred_element_type=jnp.float32)
    by_row = jnp.where(lane % SLOTS == row, packed, 0.0)
    right = dot(by_row, jnp.where(tall_row // SLOTS == tall_lane - first, 1.0, 0.0))
    by_column = jnp.where(lane // SLOTS == row - first, packed, 0.0)
    below = dot(by_column, jnp.where(tall_row % SLOTS == tall_lane, 1.0, 0.0))
    unit = jnp.where(row == lane, 1.0, 0.0)
    return jnp.where(lane >= first, right, jnp.where(row >= first, below, unit)), unit


def orthogonalize(gram, unit, first, hess):
    tile = (SLOTS, LANES)
    row, lane = iota(tile, 0), iota(tile, 1)
    down = lambda x: jnp.sum(x, axis=0, keepdims=True)
    across = lambda x: jnp.sum(x, axis=1, keepdims=True)
    fresh = (row >= first) & (row < first + STEPS)
    chain = jnp.where(fresh & (lane == row), SHIFT, 0.0) + jnp.where(fresh & (lane == row + 1), RADIUS, 0.0)
    steps = hess + chain
    old = row < first
    beta = None
    if first == 0:
        beta = jnp.sqrt(gram[0:1, 0:1] + norm_eps)
        start = 1.0 / beta
    else:
        start = jnp.ones((1, 1), jnp.float32)
    scale = jnp.where(row == first, start, jnp.where(old, 1.0, 0.0))
    coefs = unit * scale
    images = gram * scale
    column = jnp.where(row[:, 0:1] == first, start, 0.0)
    for c in range(first, first + STEPS):
        z = down(steps * column)
        products = across(images * z)
        z = z - down(coefs * products)
        column = across(unit * z)
        image = across(gram * z)
        length = jnp.sqrt(jnp.maximum(down(column * image), 0.0) + norm_eps)
        inverse = 1.0 / length
        hess_row = down(unit * products) + jnp.where(lane[0:1] == c + 1, length, 0.0)
        hess = jnp.where(row == c, hess_row, hess)
        coefs = jnp.where(row == c + 1, z * inverse, coefs)
        images = jnp.where(row == c + 1, down(gram * column) * inverse, images)
        column = column * inverse
    return coefs, hess, beta


def combine(coefs, c, parts):
    total = None
    for i, part in parts:
        term = coefs[c : c + 1, i : i + 1] * part()
        total = term if total is None else total + term
    return total


def next_kernel(first, received_ref, small_ref, drag_in_ref, old_ref, basis_in_ref, basis_ref, kept_ref, small_out_ref, send_ref, table_ref):
    edge = (basis_in_ref.shape[2] - basis_ref.shape[2]) // 2
    rows, columns = basis_ref.shape[2:]
    gram, unit = gram_matrix(received_ref, first)
    hess = small_ref[0] if first else jnp.zeros((SLOTS, LANES), jnp.float32)
    coefs, hess, beta = orthogonalize(gram, unit, first, hess)
    small_out_ref[0] = hess
    small_out_ref[1] = jnp.broadcast_to(beta, (SLOTS, LANES)) if first == 0 else small_ref[1]
    for f in range(4):
        parts = [(first + j, lambda j=j: basis_in_ref[j, f, edge : edge + rows]) for j in range(STEPS + 1)]
        if first:
            for i in range(first):
                kept_ref[i, f] = old_ref[i, f]
            parts = [(i, lambda i=i: old_ref[i, f]) for i in range(first)] + parts
        for c in range(first, first + STEPS):
            kept_ref[c, f] = combine(coefs, c, parts[: c + 1])
        basis_ref[0, f] = combine(coefs, first + STEPS, parts)
    halo = (rows - (drag_in_ref.shape[1] - 2 * HALO)) // 2
    half = (0.5 * dt_total / RADIUS) * grid_mask(rows, columns, halo)
    skip = HALO - halo
    for step in range(STEPS):
        current = [basis_ref[step, f] for f in range(4)]
        drag = [drag_in_ref[f, skip : skip + rows] for f in range(4)]
        for f, value in enumerate(power_step(current, drag, half)):
            basis_ref[step + 1, f] = value
    body = columns - LANES

    def interior(ref, j):
        return lambda: [ref[j, f, halo : rows - halo, :body] for f in range(4)]

    gram_out(
        [interior(kept_ref, i) for i in range(first + STEPS)],
        [interior(basis_ref, j) for j in range(STEPS + 1)],
        table_ref,
        send_ref,
    )


def last_kernel(first, received_ref, small_ref, old_ref, basis_ref, small_out_ref, peak_ref):
    rows, columns = basis_ref.shape[2:]
    body = columns - LANES
    halo = HALO // 2
    gram, unit = gram_matrix(received_ref, first)
    coefs, hess, _ = orthogonalize(gram, unit, first, small_ref[0])
    small_out_ref[0] = hess
    small_out_ref[1] = small_ref[1]
    small_out_ref[2] = coefs
    tiles = body // LANES
    for f in range(4):
        parts = [(i, lambda i=i: old_ref[i, f, halo : rows - halo, :body]) for i in range(first)]
        parts += [(first + j, lambda j=j: basis_ref[j, f, halo : rows - halo, :body]) for j in range(STEPS + 1)]
        peak = jnp.max(jnp.abs(combine(coefs, KRYLOV, parts)), axis=0, keepdims=True)
        for d in range(peak_ref.shape[0]):
            for t in range(tiles):
                peak_ref[d, f * tiles + t : f * tiles + t + 1, :] = peak[:, t * LANES : (t + 1) * LANES]


def finish_kernel(first, weights_ref, small_ref, state_ref, old_ref, basis_ref, peaks_ref, combined_ref, error_ref):
    rows, columns = basis_ref.shape[2:]
    body = columns - LANES
    halo = HALO // 2
    hess, beta, coefs = small_ref[0], small_ref[1, 0:1, 0:1], small_ref[2]
    dot = functools.partial(jnp.dot, precision=HIGH, preferred_element_type=jnp.float32)
    size = SUBSTEPS * SLOTS
    row, lane = iota((size, LANES), 0), iota((size, LANES), 1)
    row_in, lane_in = row % SLOTS, lane % SLOTS
    same = (row // SLOTS == lane // SLOTS) & (lane < size)
    spread = jnp.where(iota((LANES, LANES), 0) == iota((LANES, LANES), 1) % SLOTS, 1.0, 0.0)
    wide = dot(jnp.concatenate([hess] * SUBSTEPS, axis=0), spread)
    fraction = ((row // SLOTS) + 1).astype(jnp.float32) * (1.0 / SUBSTEPS)
    scaled = jnp.where(same & (row_in < KRYLOV) & (lane_in < KRYLOV), wide * fraction, 0.0)
    scaled = scaled + jnp.where(same & (row_in == KRYLOV) & (lane_in == 0), 1.0, 0.0)
    scaled = scaled * (1.0 / 2.0**squarings)
    unit = jnp.where(row == lane, 1.0, 0.0)
    pad = jnp.zeros((LANES - size, LANES), jnp.float32)

    def times(a, b):
        return dot(a, jnp.concatenate([b, pad], axis=0))

    result, term = unit, unit
    for degree in range(1, taylor_degree + 1):
        term = times(term, scaled) * (1.0 / degree)
        result = result + term
    for _ in range(squarings):
        result = times(result, result)
    mixing = jnp.zeros((1, LANES), jnp.float32)
    highest = jnp.zeros((1, 1), jnp.float32)
    gather = jnp.where(iota((LANES, LANES), 0) % SLOTS == iota((LANES, LANES), 1), 1.0, 0.0)
    for k in range(SUBSTEPS):
        tau = (k + 1) / SUBSTEPS
        factor = dt_total * tau
        g = result[k * SLOTS + KRYLOV : k * SLOTS + KRYLOV + 1, :]
        mixing = mixing + jnp.where(lane[0:1] // SLOTS == k, weights_ref[k] * factor, 0.0) * beta * g
        last = jnp.abs(g[:, k * SLOTS + KRYLOV - 1 : k * SLOTS + KRYLOV])
        estimate = (factor * tau) * beta * hess[KRYLOV - 1 : KRYLOV, KRYLOV : KRYLOV + 1] * last
        highest = jnp.maximum(highest, estimate)
    mixing = jnp.where(lane_in[0:1] < KRYLOV, mixing, 0.0)
    mixing = dot(jnp.broadcast_to(mixing, (8, LANES)), gather)
    coef_pad = jnp.concatenate([coefs, jnp.zeros((LANES - SLOTS, LANES), jnp.float32)], axis=0)
    share = dot(jnp.where(iota((8, LANES), 1) < KRYLOV, mixing, 0.0), coef_pad)
    for f in range(4):
        parts = [(i, lambda i=i: old_ref[i, f, halo : rows - halo, :body]) for i in range(first)]
        parts += [(first + j, lambda j=j: basis_ref[j, f, halo : rows - halo, :body]) for j in range(STEPS + 1)]
        combined_ref[f] = state_ref[f] + combine(share, 0, parts)
    peak = jnp.max(peaks_ref[...], axis=0) * highest
    tiles = body // LANES
    for f in range(4):
        for t in range(tiles):
            error_ref[f : f + 1, t * LANES : (t + 1) * LANES] = peak[f * tiles + t : f * tiles + t + 1]


def shards(state, damping, weights):
    fields, height, width = state.shape
    body = width
    columns = width + LANES
    devices = lax.axis_size("sub") * lax.axis_size("gx") * lax.axis_size("gy")
    lines = lax.axis_size("sub") * lax.axis_size("gx")
    sides = lax.axis_size("gy")
    f32 = functools.partial(jax.ShapeDtypeStruct, dtype=jnp.float32)
    near = lambda shape: pltpu.VMEM(shape, jnp.float32)
    pair = jnp.stack([state, damping])
    head, tail = pair[..., :LANES], pair[..., body - LANES :]
    if sides == 2:
        halo = lax.ppermute(jnp.where(lax.axis_index("gy") == 0, tail, head), "gy", [(0, 1), (1, 0)])
    else:
        from_right = lax.ppermute(head, "gy", [((i + 1) % sides, i) for i in range(sides)])
        from_left = lax.ppermute(tail, "gy", [(i, (i + 1) % sides) for i in range(sides)])
        halo = jnp.concatenate([from_right[..., : LANES // 2], from_left[..., LANES // 2 :]], axis=-1)
    own = jnp.concatenate([pair, halo], axis=-1)
    up = lax.ppermute(own[:, :, height - HALO :], ROWS, [(i, (i + 1) % lines) for i in range(lines)])
    down = lax.ppermute(own[:, :, :HALO], ROWS, [((i + 1) % lines, i) for i in range(lines)])

    def call(body_fn, outs, *args, smem=(), scratch=()):
        specs = [pl.BlockSpec(memory_space=pltpu.SMEM) if k in smem else VMEM for k in range(len(args))]
        args = [a if k in smem else pltpu.with_memory_space_constraint(a, pltpu.VMEM) for k, a in enumerate(args)]
        return pl.pallas_call(
            body_fn,
            out_shape=outs,
            in_specs=specs,
            out_specs=[VMEM] * len(outs),
            scratch_shapes=list(scratch),
            compiler_params=pltpu.CompilerParams(vmem_limit_bytes=16 * 2**20),
        )(*args)

    table = pltpu.VMEM((LANES, LANES), jnp.float32)
    send_shape = near((devices, 1, LANES))
    small_shape = near((2, SLOTS, LANES))
    tall = height + 2 * HALO
    short = height + HALO
    basis, drag, send = call(
        first_kernel,
        [near((STEPS + 1, fields, tall, columns)), near((fields, tall, columns)), send_shape],
        own,
        up,
        down,
        scratch=[table],
    )
    exchange = lambda x, axes: lax.all_to_all(x, axes, 0, 0)
    received = exchange(send, ALL)
    small = jnp.zeros((2, SLOTS, LANES), jnp.float32)
    kept = drag
    for first in range(0, KRYLOV - STEPS, STEPS):
        basis, kept, small, send = call(
            functools.partial(next_kernel, first),
            [
                near((STEPS + 1, fields, short, columns)),
                near((first + STEPS, fields, short, columns)),
                small_shape,
                send_shape,
            ],
            received,
            small,
            drag,
            kept,
            basis,
            scratch=[table],
        )
        received = exchange(send, ALL)
    first = KRYLOV - STEPS
    peak_rows = fields * (body // LANES)
    small, peaks = call(
        functools.partial(last_kernel, first),
        [near((3, SLOTS, LANES)), near((lines, peak_rows, LANES))],
        received,
        small,
        kept,
        basis,
    )
    peaks = exchange(peaks, ROWS)
    combined, column_error = call(
        functools.partial(finish_kernel, first),
        [f32((fields, height, width)), f32((fields, width))],
        weights,
        small,
        state,
        kept,
        basis,
        peaks,
        smem=(0,),
    )
    return combined, column_error


def solution(mesh):
    return jax.shard_map(
        shards,
        mesh=mesh,
        in_specs=(P(None, ROWS, "gy"), P(None, ROWS, "gy"), P()),
        out_specs=(P(None, ROWS, "gy"), P(None, "gy")),
        check_vma=False,
    )
```

```python
import functools
import math

import jax
import jax.numpy as jnp
from jax import lax
from jax.experimental import pallas as pl
from jax.experimental.pallas import tpu as pltpu
from jax.sharding import PartitionSpec as P

KRYLOV = 12
SUBSTEPS = 4
BLOCKS = (5, 7)
HALO = 16
LANES = 128
SLOTS = 16
EDGE = 16

dt_total = 4.0
buoyancy_sq = 0.5
norm_eps = 1e-06
taylor_degree = 12
squarings = 8
SHIFT = -2.0
RADIUS = 4.0

ROWS = ("sub", "gx")
ALL = ("sub", "gx", "gy")
HIGH = lax.Precision.HIGHEST
VMEM = pl.BlockSpec(memory_space=pltpu.VMEM)


def iota(shape, dim):
    return lax.broadcasted_iota(jnp.int32, shape, dim)


def rise_rows(x):
    return pltpu.roll(x, x.shape[0] - 1, 0) - pltpu.roll(x, 1, 0)


def rise_columns(x):
    return pltpu.roll(x, x.shape[1] - 1, 1) - pltpu.roll(x, 1, 1)


def grid_mask(rows, columns, halo_rows):
    line, lane = iota((rows, columns), 0), iota((rows, columns), 1)
    place = lax.axis_index("sub") * lax.axis_size("gx") + lax.axis_index("gx")
    last = lax.axis_size("sub") * lax.axis_size("gx") - 1
    side = lax.axis_index("gy")
    first_line = jnp.where(place > 0, 0, halo_rows)
    end_line = jnp.where(place < last, rows, rows - halo_rows)
    body = columns - LANES
    right_end = jnp.where(side < lax.axis_size("gy") - 1, body + EDGE, body)
    left_start = jnp.where(side > 0, columns - EDGE, columns)
    inside = (line >= first_line) & (line < end_line) & ((lane < right_end) | (lane >= left_start))
    return jnp.where(inside, 1.0, 0.0)


def power_step(fields, drag, half):
    vx, vy, b, p = fields
    quarter = dt_total / RADIUS
    return (
        -half * rise_rows(p) - drag[0] * vx,
        -half * rise_columns(p) + quarter * b - drag[1] * vy,
        (-buoyancy_sq * quarter) * vy - drag[2] * b,
        -half * (rise_rows(vx) + rise_columns(vy)) - drag[3] * p,
    )


def two_sum(a, b):
    total = a + b
    part = total - a
    return total, (a - (total - part)) + (b - part)


def pair_sum(one, two):
    total, error = two_sum(one[0], two[0])
    return total, one[1] + two[1] + error


def split(a):
    scaled = 4097.0 * a
    high = scaled - (scaled - a)
    return high, a - high


def add_product(total, a, b, b_parts):
    product = a * b
    a_high, a_low = split(a)
    error = ((a_high * b_parts[0] - product) + a_high * b_parts[1] + a_low * b_parts[0]) + a_low * b_parts[1]
    high, rest = two_sum(total[0], product)
    return high, total[1] + (rest + error)


def tree_sum(tiles):
    while len(tiles) > 1:
        tiles = [pair_sum(tiles[k], tiles[k + 1]) for k in range(0, len(tiles) - 1, 2)] + tiles[len(tiles) // 2 * 2 :]
    total = tiles[0]
    for shift in (4, 2, 1):
        total = pair_sum(total, (pltpu.roll(total[0], shift, 0), pltpu.roll(total[1], shift, 0)))
    return total


def pair_rows(one, two):
    total = None
    for f in range(4):
        prod = one[f] * two[f]
        part = None
        for r in range(0, prod.shape[0], 8):
            for c in range(0, prod.shape[1], LANES):
                tile = prod[r : r + 8, c : c + LANES]
                part = tile if part is None else part + tile
        total = part if total is None else total + part
    return jnp.sum(total, axis=0, keepdims=True)


def gram_out(old, new, table_ref, send_ref):
    first = len(old)
    table_ref[...] = jnp.zeros_like(table_ref)
    for j in range(len(new)):
        for i in range(first):
            table_ref[j * SLOTS + i : j * SLOTS + i + 1, :] = pair_rows(old[i](), new[j]())
        for i in range(j + 1):
            row = pair_rows(new[i](), new[j]())
            table_ref[j * SLOTS + first + i : j * SLOTS + first + i + 1, :] = row
            if i != j:
                table_ref[i * SLOTS + first + j : i * SLOTS + first + j + 1, :] = row
    turned = jnp.transpose(table_ref[...])
    zero = jnp.zeros((8, LANES), jnp.float32)
    high, low = tree_sum([(turned[r : r + 8], zero) for r in range(0, LANES, 8)])
    for d in range(send_ref.shape[0]):
        send_ref[d, 0:1] = high[0:1]
        send_ref[d, 1:2] = low[0:1]


def edge_kernel(state_ref, damping_ref, *edge_refs):
    width = state_ref.shape[2]
    lane = iota((state_ref.shape[1], LANES), 1)

    def packed(pick):
        total = None
        for k in range(8):
            ref = state_ref if k < 4 else damping_ref
            head, tail = ref[k % 4, :, :LANES], ref[k % 4, :, width - LANES :]
            tile = pltpu.roll(pick(head, pltpu.roll(tail, EDGE, 1)), k * EDGE, 1) if k else pick(head, pltpu.roll(tail, EDGE, 1))
            total = tile if total is None else jnp.where(lane // EDGE == k, tile, total)
        return total

    if len(edge_refs) == 1:
        left = lax.axis_index("gy") == 0
        edge_refs[0][...] = packed(lambda head, tail: jnp.where(left, tail, head))
    else:
        edge_refs[0][...] = packed(lambda head, tail: head)
        edge_refs[1][...] = packed(lambda head, tail: tail)


def pack_kernel(count, state_ref, damping_ref, *refs):
    halo_refs, out_refs = refs[:count], refs[count:]
    height, width = state_ref.shape[1:]
    for out_ref, start in zip(out_refs, (height - HALO, 0)):
        lines = slice(start, start + HALO)
        at = 0
        for k in range(8):
            ref = state_ref if k < 4 else damping_ref
            for c in range(0, width, LANES):
                out_ref[at : at + HALO] = ref[k % 4, lines, c : c + LANES]
                at += HALO
        for halo_ref in halo_refs:
            out_ref[at : at + HALO] = halo_ref[lines]
            at += HALO


def first_kernel(count, state_ref, damping_ref, *refs):
    halo_refs = refs[:count]
    up_ref, down_ref, basis_ref, drag_ref, send_ref, table_ref = refs[count:]
    height, width = state_ref.shape[1:]
    rows, columns = height + 2 * HALO, width + LANES
    tiles = width // LANES
    mask = grid_mask(rows, columns, HALO)

    def side_tile(k, right, left):
        lane = iota(right.shape, 1)
        right = pltpu.roll(right, LANES - k * EDGE, 1) if k else right
        return jnp.where(lane < LANES // 2, right, pltpu.roll(left, LANES - (k + 1) * EDGE, 1) if k < 7 else left)

    def neighbour(ref, k):
        parts = [ref[(k * tiles + t) * HALO : (k * tiles + t + 1) * HALO] for t in range(tiles)]
        at = 8 * tiles * HALO
        ends = [ref[at + c * HALO : at + (c + 1) * HALO] for c in range(count)]
        return jnp.concatenate(parts + [side_tile(k, ends[0], ends[-1])], axis=1)

    def whole(k):
        ref = state_ref if k < 4 else damping_ref
        own = jnp.concatenate([ref[k % 4], side_tile(k, halo_refs[0][...], halo_refs[-1][...])], axis=1)
        joined = jnp.concatenate([neighbour(up_ref, k), own, neighbour(down_ref, k)], axis=0)
        return jnp.where(mask > 0, joined, 0.0)

    state = [whole(f) for f in range(4)]
    damping = [whole(4 + f) for f in range(4)]
    vx, vy, b, p = state
    half = 0.5 * mask
    linear = (
        -half * rise_rows(p),
        -half * rise_columns(p) + b,
        -buoyancy_sq * vy,
        -half * (rise_rows(vx) + rise_columns(vy)),
    )
    for f in range(4):
        square = damping[f] * state[f] * state[f]
        basis_ref[0, f] = linear[f] - square * state[f]
        drag_ref[f] = (3.0 * dt_total / RADIUS) * square
    half = (0.5 * dt_total / RADIUS) * mask
    drag = [drag_ref[f] + SHIFT / RADIUS for f in range(4)]
    steps = BLOCKS[0]
    for step in range(steps):
        current = [basis_ref[step, f] for f in range(4)]
        for f, value in enumerate(power_step(current, drag, half)):
            basis_ref[step + 1, f] = value

    def interior(j):
        return lambda: [basis_ref[j, f, HALO : rows - HALO, :width] for f in range(4)]

    gram_out([], [interior(j) for j in range(steps + 1)], table_ref, send_ref)


dot = functools.partial(jnp.dot, precision=HIGH, preferred_element_type=jnp.float32)
TILE = (SLOTS, LANES)


def tall(x):
    return jnp.concatenate([x, jnp.zeros((LANES - x.shape[0], LANES), jnp.float32)], axis=0)


def down_sum(x):
    return jnp.sum(x, axis=0, keepdims=True)


def across_sum(x):
    return jnp.sum(x, axis=1, keepdims=True)


def gram_matrix(received_ref, first):
    devices = received_ref.shape[0]
    parts = [(received_ref[d : d + 8, 0, :], received_ref[d : d + 8, 1, :]) for d in range(0, devices, 8)]
    packed = jnp.concatenate([jnp.concatenate([part, part], axis=0) for part in tree_sum(parts)], axis=0)
    row, lane = iota((2 * SLOTS, LANES), 0) % SLOTS, iota((2 * SLOTS, LANES), 1)
    tall_row, tall_lane = iota((LANES, LANES), 0), iota((LANES, LANES), 1)
    by_row = jnp.where(lane % SLOTS == row, packed, 0.0)
    right = dot(by_row, jnp.where(tall_row // SLOTS == tall_lane - first, 1.0, 0.0))
    by_column = jnp.where(lane // SLOTS == row - first, packed, 0.0)
    below = dot(by_column, jnp.where((tall_row % SLOTS == tall_lane) & (tall_lane < SLOTS), 1.0, 0.0))
    both = jnp.where(lane >= first, right, jnp.where(row >= first, below, 0.0))
    return both[:SLOTS] + old_unit(first), both[SLOTS:]


def old_unit(first):
    row, lane = iota(TILE, 0), iota(TILE, 1)
    return jnp.where((row == lane) & (row < first), 1.0, 0.0)


def gram_schmidt(gram, steps, start, hess, first, count):
    row, lane = iota(TILE, 0), iota(TILE, 1)
    unit = jnp.where(row == lane, 1.0, 0.0)
    scale = jnp.where(row == first, start, jnp.where(row < first, 1.0, 0.0))
    coefs = unit * scale
    images = gram * scale
    column = jnp.where(row[:, 0:1] == first, start, 0.0)
    for c in range(first, first + count):
        z = down_sum(steps * column)
        products = across_sum(images * z)
        z = z - down_sum(coefs * products)
        column = across_sum(unit * z)
        image = across_sum(gram * z)
        length = jnp.sqrt(jnp.maximum(down_sum(column * image), 0.0) + norm_eps)
        inverse = 1.0 / length
        hess_row = down_sum(unit * products) + jnp.where(lane[0:1] == c + 1, length, 0.0)
        hess = jnp.where(row == c, hess_row, hess)
        coefs = jnp.where(row == c + 1, z * inverse, coefs)
        images = jnp.where(row == c + 1, down_sum(gram * column) * inverse, images)
        column = column * inverse
    return coefs, hess


def refined_gram(coefs, gram, gram_low, first, count):
    row, lane = iota(TILE, 0), iota(TILE, 1)
    slots = range(first + count + 1)
    gram_parts = split(gram)
    zero = jnp.zeros(TILE, jnp.float32)
    image = (zero, zero)
    for j in slots:
        line = slice(j, j + 1)
        column = coefs[:, line]
        image = add_product(image, column, gram[line], [part[line] for part in gram_parts])
        image = image[0], image[1] + column * gram_low[line]
    turned = dot(jnp.where(row == lane, 1.0, 0.0), jnp.transpose(tall(coefs)))
    turned_parts = split(turned)
    result = (zero, zero)
    for i in slots:
        line = slice(i, i + 1)
        result = add_product(result, image[0][:, line], turned[line], [part[line] for part in turned_parts])
        result = result[0], result[1] + image[1][:, line] * turned[line]
    inner = (row < first) & (lane < first)
    return jnp.where(inner, old_unit(first), result[0] + result[1])


def basis_terms(hess, first):
    if first == 0:
        return jnp.full((1, 1), SHIFT, jnp.float32), jnp.zeros((1, 1), jnp.float32)
    c = first - 1
    shift = 0.5 * (hess[c - 1 : c, c - 1 : c] + hess[c : c + 1, c : c + 1])
    return shift, hess[c : c + 1, c - 1 : c]


def orthogonalize(received_ref, hess, first, count):
    gram, gram_low = gram_matrix(received_ref, first)
    row, lane = iota(TILE, 0), iota(TILE, 1)
    shift, back = basis_terms(hess, first)
    fresh = (row >= first) & (row < first + count)
    chain = jnp.where(lane == row, shift, 0.0) + jnp.where(lane == row + 1, RADIUS, 0.0)
    chain = chain + jnp.where((lane == row - 1) & (row > first), back, 0.0)
    steps = hess + jnp.where(fresh, chain, 0.0)
    one = jnp.ones((1, 1), jnp.float32)
    beta = jnp.sqrt(gram[0:1, 0:1] + norm_eps)
    coefs, image = gram_schmidt(gram, steps, one if first else 1.0 / beta, hess, first, count)
    gram = refined_gram(coefs, gram, gram_low, first, count)
    again, hess = gram_schmidt(gram, image, one, hess, first, count)
    return dot(again, tall(coefs)), hess, beta


def combine(coefs, c, parts):
    total = None
    for i, part in parts:
        term = coefs[c : c + 1, i : i + 1] * part()
        total = term if total is None else total + term
    return total


def middle_kernel(received_ref, drag_in_ref, basis_in_ref, basis_ref, kept_ref, small_ref, send_ref, table_ref):
    first, count = BLOCKS
    rows, columns = basis_ref.shape[2:]
    edge = (basis_in_ref.shape[2] - rows) // 2
    halo = HALO - edge
    body = columns - LANES
    coefs, hess, beta = orthogonalize(received_ref, jnp.zeros(TILE, jnp.float32), 0, first)
    small_ref[0] = hess
    small_ref[1] = jnp.broadcast_to(beta, TILE)
    for f in range(4):
        inner = [(j, lambda j=j: basis_in_ref[j, f, HALO : edge + rows - halo, :body]) for j in range(first + 1)]
        for c in range(first):
            kept_ref[c, f] = combine(coefs, c, inner[: c + 1])
        outer = [(j, lambda j=j: basis_in_ref[j, f, edge : edge + rows]) for j in range(first + 1)]
        basis_ref[0, f] = combine(coefs, first, outer)
    shift, back = basis_terms(hess, first)
    back = back * (1.0 / RADIUS)
    half = (0.5 * dt_total / RADIUS) * grid_mask(rows, columns, halo)
    drag = [drag_in_ref[f, edge : edge + rows] + shift * (1.0 / RADIUS) for f in range(4)]
    for step in range(count):
        current = [basis_ref[step, f] for f in range(4)]
        for f, value in enumerate(power_step(current, drag, half)):
            basis_ref[step + 1, f] = value - back * basis_ref[step - 1, f] if step else value

    def interior(ref, j, lines):
        return lambda: [ref[j, f, lines, :body] for f in range(4)]

    gram_out(
        [interior(kept_ref, i, slice(None)) for i in range(first)],
        [interior(basis_ref, j, slice(halo, rows - halo)) for j in range(count + 1)],
        table_ref,
        send_ref,
    )


def block_parts(kept_ref, basis_ref, f):
    first, count = BLOCKS
    height, body = kept_ref.shape[2:]
    halo = (basis_ref.shape[2] - height) // 2
    parts = [(i, lambda i=i: kept_ref[i, f]) for i in range(first)]
    return parts + [(first + j, lambda j=j: basis_ref[j, f, halo : halo + height, :body]) for j in range(count + 1)]


def last_kernel(received_ref, small_ref, kept_ref, basis_ref, small_out_ref, peak_ref):
    body = kept_ref.shape[3]
    coefs, hess, _ = orthogonalize(received_ref, small_ref[0], *BLOCKS)
    small_out_ref[0] = hess
    small_out_ref[1] = small_ref[1]
    small_out_ref[2] = coefs
    tiles = body // LANES
    for f in range(4):
        peak = jnp.max(jnp.abs(combine(coefs, KRYLOV, block_parts(kept_ref, basis_ref, f))), axis=0, keepdims=True)
        for d in range(peak_ref.shape[0]):
            for t in range(tiles):
                peak_ref[d, f * tiles + t : f * tiles + t + 1, :] = peak[:, t * LANES : (t + 1) * LANES]


def finish_kernel(weights_ref, small_ref, state_ref, kept_ref, basis_ref, peaks_ref, combined_ref, error_ref):
    body = kept_ref.shape[3]
    hess, beta, coefs = small_ref[0], small_ref[1, 0:1, 0:1], small_ref[2]
    size = SUBSTEPS * SLOTS
    row, lane = iota((size, LANES), 0), iota((size, LANES), 1)
    row_in, lane_in = row % SLOTS, lane % SLOTS
    same = (row // SLOTS == lane // SLOTS) & (lane < size)
    lower = jnp.where((row_in < KRYLOV) & (lane < KRYLOV), jnp.concatenate([hess] * SUBSTEPS, axis=0), 0.0)
    wide = lower
    for k in range(1, SUBSTEPS):
        wide = jnp.where(lane // SLOTS == k, pltpu.roll(lower, k * SLOTS, 1), wide)
    fraction = ((row // SLOTS) + 1).astype(jnp.float32) * (1.0 / SUBSTEPS)
    scaled = jnp.where(same, wide * fraction, 0.0)
    scaled = scaled + jnp.where(same & (row_in == KRYLOV) & (lane_in == 0), 1.0, 0.0)
    scaled = scaled * (1.0 / 2.0**squarings)
    unit = jnp.where(row == lane, 1.0, 0.0)

    def times(a, b):
        return dot(a, tall(b))

    power = [unit, scaled, times(scaled, scaled)]
    power += [times(power[2], scaled), times(power[2], power[2])]

    def group(k, count):
        total = None
        for i in range(count):
            term = power[i] * (1.0 / math.factorial(k + i))
            total = term if total is None else total + term
        return total

    top = taylor_degree - 4
    result = group(top, 5)
    while top > 0:
        top -= 4
        result = times(result, power[4]) + group(top, 4)
    for _ in range(squarings):
        result = times(result, result)
    mixing = jnp.zeros((1, LANES), jnp.float32)
    highest = jnp.zeros((1, 1), jnp.float32)
    for k in range(SUBSTEPS):
        tau = (k + 1) / SUBSTEPS
        factor = dt_total * tau
        g = result[k * SLOTS + KRYLOV : k * SLOTS + KRYLOV + 1, :]
        g = pltpu.roll(g, LANES - k * SLOTS, 1) if k else g
        mixing = mixing + weights_ref[k] * factor * beta * g
        estimate = (factor * tau) * beta * hess[KRYLOV - 1 : KRYLOV, KRYLOV : KRYLOV + 1] * jnp.abs(g[:, KRYLOV - 1 : KRYLOV])
        highest = jnp.maximum(highest, estimate)
    mixing = jnp.where(lane[0:8] < KRYLOV, jnp.broadcast_to(mixing, (8, LANES)), 0.0)
    share = dot(mixing, tall(coefs))
    for f in range(4):
        combined_ref[f] = state_ref[f] + combine(share, 0, block_parts(kept_ref, basis_ref, f))
    peak = jnp.max(peaks_ref[...], axis=0) * highest
    tiles = body // LANES
    for f in range(4):
        for t in range(tiles):
            error_ref[f : f + 1, t * LANES : (t + 1) * LANES] = peak[f * tiles + t : f * tiles + t + 1]


def shards(state, damping, weights):
    fields, height, width = state.shape
    columns = width + LANES
    lines = lax.axis_size("sub") * lax.axis_size("gx")
    sides = lax.axis_size("gy")
    devices = lines * sides
    f32 = lambda *shape: jax.ShapeDtypeStruct(shape, jnp.float32)
    near = lambda *shape: pltpu.VMEM(shape, jnp.float32)

    def call(kernel, outs, *args, smem=(), scratch=()):
        specs = [pl.BlockSpec(memory_space=pltpu.SMEM) if k in smem else VMEM for k in range(len(args))]
        args = [a if k in smem else pltpu.with_memory_space_constraint(a, pltpu.VMEM) for k, a in enumerate(args)]
        return pl.pallas_call(
            kernel,
            out_shape=outs,
            in_specs=specs,
            out_specs=[VMEM] * len(outs),
            scratch_shapes=list(scratch),
            compiler_params=pltpu.CompilerParams(vmem_limit_bytes=16 * 2**20),
        )(*args)

    exchange = lambda x, axes: lax.all_to_all(x, axes, 0, 0)
    table = near(LANES, LANES)
    send_shape = near(devices, 2, LANES)
    short = height + HALO
    first, count = BLOCKS

    edges = call(edge_kernel, [near(height, LANES)] * (1 if sides == 2 else 2), state, damping)
    if sides == 2:
        halos = [lax.ppermute(edges[0], "gy", [(0, 1), (1, 0)])]
    else:
        halos = [
            lax.ppermute(edges[0], "gy", [((i + 1) % sides, i) for i in range(sides)]),
            lax.ppermute(edges[1], "gy", [(i, (i + 1) % sides) for i in range(sides)]),
        ]
    number = len(halos)
    stack = (8 * (width // LANES) + number) * HALO
    packs = call(
        functools.partial(pack_kernel, number),
        [near(stack, LANES)] * (1 if height == HALO else 2),
        state,
        damping,
        *halos,
    )
    up = lax.ppermute(packs[0], ROWS, [(i, (i + 1) % lines) for i in range(lines)])
    down = lax.ppermute(packs[-1], ROWS, [((i + 1) % lines, i) for i in range(lines)])
    tall_rows = height + 2 * HALO
    basis, drag, send = call(
        functools.partial(first_kernel, number),
        [near(first + 1, fields, tall_rows, columns), near(fields, tall_rows, columns), send_shape],
        state,
        damping,
        *halos,
        up,
        down,
        scratch=[table],
    )
    basis, kept, small, send = call(
        middle_kernel,
        [near(count + 1, fields, short, columns), near(first, fields, height, width), near(2, *TILE), send_shape],
        exchange(send, ALL),
        drag,
        basis,
        scratch=[table],
    )
    small, peaks = call(
        last_kernel,
        [near(3, *TILE), near(lines, fields * (width // LANES), LANES)],
        exchange(send, ALL),
        small,
        kept,
        basis,
    )
    combined, column_error = call(
        finish_kernel,
        [f32(fields, height, width), f32(fields, width)],
        weights,
        small,
        state,
        kept,
        basis,
        exchange(peaks, ROWS),
        smem=(0,),
    )
    return combined, column_error


def solution(mesh):
    return jax.shard_map(
        shards,
        mesh=mesh,
        in_specs=(P(None, ROWS, "gy"), P(None, ROWS, "gy"), P()),
        out_specs=(P(None, ROWS, "gy"), P(None, "gy")),
        check_vma=False,
    )
```

```python
import functools
import math

import jax
import jax.numpy as jnp
from jax import lax
from jax.experimental import pallas as pl
from jax.experimental.pallas import tpu as pltpu
from jax.sharding import PartitionSpec as P

KRYLOV = 12
SUBSTEPS = 4
BLOCKS = (6, 6)
HALO = 16
LANES = 128
SLOTS = 16
EDGE = 16

dt_total = 4.0
buoyancy_sq = 0.5
norm_eps = 1e-06
taylor_degree = 12
squarings = 8
SHIFT = -2.0
RADIUS = 4.0

ROWS = ("sub", "gx")
ALL = ("sub", "gx", "gy")
HIGH = lax.Precision.HIGHEST
VMEM = pl.BlockSpec(memory_space=pltpu.VMEM)


def iota(shape, dim):
    return lax.broadcasted_iota(jnp.int32, shape, dim)


def rise_rows(x):
    return pltpu.roll(x, x.shape[0] - 1, 0) - pltpu.roll(x, 1, 0)


def rise_columns(x):
    return pltpu.roll(x, x.shape[1] - 1, 1) - pltpu.roll(x, 1, 1)


def grid_mask(rows, columns, halo_rows):
    line, lane = iota((rows, columns), 0), iota((rows, columns), 1)
    place = lax.axis_index("sub") * lax.axis_size("gx") + lax.axis_index("gx")
    last = lax.axis_size("sub") * lax.axis_size("gx") - 1
    side = lax.axis_index("gy")
    first_line = jnp.where(place > 0, 0, halo_rows)
    end_line = jnp.where(place < last, rows, rows - halo_rows)
    body = columns - LANES
    right_end = jnp.where(side < lax.axis_size("gy") - 1, body + EDGE, body)
    left_start = jnp.where(side > 0, columns - EDGE, columns)
    inside = (line >= first_line) & (line < end_line) & ((lane < right_end) | (lane >= left_start))
    return jnp.where(inside, 1.0, 0.0)


def power_step(fields, drag, half):
    vx, vy, b, p = fields
    quarter = dt_total / RADIUS
    return (
        -half * rise_rows(p) - drag[0] * vx,
        -half * rise_columns(p) + quarter * b - drag[1] * vy,
        (-buoyancy_sq * quarter) * vy - drag[2] * b,
        -half * (rise_rows(vx) + rise_columns(vy)) - drag[3] * p,
    )


def two_sum(a, b):
    total = a + b
    part = total - a
    return total, (a - (total - part)) + (b - part)


def pair_sum(one, two):
    total, error = two_sum(one[0], two[0])
    return total, one[1] + two[1] + error


def split(a):
    scaled = 4097.0 * a
    high = scaled - (scaled - a)
    return high, a - high


def add_product(total, a, b, b_parts):
    product = a * b
    a_high, a_low = split(a)
    error = ((a_high * b_parts[0] - product) + a_high * b_parts[1] + a_low * b_parts[0]) + a_low * b_parts[1]
    high, rest = two_sum(total[0], product)
    return high, total[1] + (rest + error)


def tree_sum(tiles):
    while len(tiles) > 1:
        tiles = [pair_sum(tiles[k], tiles[k + 1]) for k in range(0, len(tiles) - 1, 2)] + tiles[len(tiles) // 2 * 2 :]
    total = tiles[0]
    for shift in (4, 2, 1):
        total = pair_sum(total, (pltpu.roll(total[0], shift, 0), pltpu.roll(total[1], shift, 0)))
    return total


def pair_rows(one, two):
    total = None
    for f in range(4):
        prod = one[f] * two[f]
        part = None
        for r in range(0, prod.shape[0], 8):
            for c in range(0, prod.shape[1], LANES):
                tile = prod[r : r + 8, c : c + LANES]
                part = tile if part is None else part + tile
        total = part if total is None else total + part
    return jnp.sum(total, axis=0, keepdims=True)


def gram_out(old, new, table_ref, send_ref):
    first = len(old)
    table_ref[...] = jnp.zeros_like(table_ref)
    for j in range(len(new)):
        for i in range(first):
            table_ref[j * SLOTS + i : j * SLOTS + i + 1, :] = pair_rows(old[i](), new[j]())
        for i in range(j + 1):
            row = pair_rows(new[i](), new[j]())
            table_ref[j * SLOTS + first + i : j * SLOTS + first + i + 1, :] = row
            if i != j:
                table_ref[i * SLOTS + first + j : i * SLOTS + first + j + 1, :] = row
    turned = jnp.transpose(table_ref[...])
    zero = jnp.zeros((8, LANES), jnp.float32)
    high, low = tree_sum([(turned[r : r + 8], zero) for r in range(0, LANES, 8)])
    for d in range(send_ref.shape[0]):
        send_ref[d, 0:1] = high[0:1]
        send_ref[d, 1:2] = low[0:1]


def edge_kernel(far_state_ref, far_damping_ref, state_ref, damping_ref, *refs):
    edge_refs, semaphores = refs[:-1], refs[-1]
    copies = [
        pltpu.make_async_copy(far_state_ref, state_ref, semaphores.at[0]),
        pltpu.make_async_copy(far_damping_ref, damping_ref, semaphores.at[1]),
    ]
    for copy in copies:
        copy.start()
    for copy in copies:
        copy.wait()
    width = state_ref.shape[2]
    lane = iota((state_ref.shape[1], LANES), 1)

    def packed(pick):
        total = None
        for k in range(8):
            ref = state_ref if k < 4 else damping_ref
            head, tail = ref[k % 4, :, :LANES], ref[k % 4, :, width - LANES :]
            tile = pltpu.roll(pick(head, pltpu.roll(tail, EDGE, 1)), k * EDGE, 1) if k else pick(head, pltpu.roll(tail, EDGE, 1))
            total = tile if total is None else jnp.where(lane // EDGE == k, tile, total)
        return total

    if len(edge_refs) == 1:
        left = lax.axis_index("gy") == 0
        edge_refs[0][...] = packed(lambda head, tail: jnp.where(left, tail, head))
    else:
        edge_refs[0][...] = packed(lambda head, tail: head)
        edge_refs[1][...] = packed(lambda head, tail: tail)


def pack_kernel(count, state_ref, damping_ref, *refs):
    halo_refs, out_refs = refs[:count], refs[count:]
    height, width = state_ref.shape[1:]
    for out_ref, start in zip(out_refs, (height - HALO, 0)):
        lines = slice(start, start + HALO)
        at = 0
        for k in range(8):
            ref = state_ref if k < 4 else damping_ref
            for c in range(0, width, LANES):
                out_ref[at : at + HALO] = ref[k % 4, lines, c : c + LANES]
                at += HALO
        for halo_ref in halo_refs:
            out_ref[at : at + HALO] = halo_ref[lines]
            at += HALO


def first_kernel(count, state_ref, damping_ref, *refs):
    halo_refs = refs[:count]
    up_ref, down_ref, basis_ref, drag_ref, send_ref, table_ref = refs[count:]
    height, width = state_ref.shape[1:]
    rows, columns = height + 2 * HALO, width + LANES
    tiles = width // LANES
    mask = grid_mask(rows, columns, HALO)

    def side_tile(k, right, left):
        lane = iota(right.shape, 1)
        right = pltpu.roll(right, LANES - k * EDGE, 1) if k else right
        return jnp.where(lane < LANES // 2, right, pltpu.roll(left, LANES - (k + 1) * EDGE, 1) if k < 7 else left)

    def neighbour(ref, k):
        parts = [ref[(k * tiles + t) * HALO : (k * tiles + t + 1) * HALO] for t in range(tiles)]
        at = 8 * tiles * HALO
        ends = [ref[at + c * HALO : at + (c + 1) * HALO] for c in range(count)]
        return jnp.concatenate(parts + [side_tile(k, ends[0], ends[-1])], axis=1)

    def whole(k):
        ref = state_ref if k < 4 else damping_ref
        own = jnp.concatenate([ref[k % 4], side_tile(k, halo_refs[0][...], halo_refs[-1][...])], axis=1)
        joined = jnp.concatenate([neighbour(up_ref, k), own, neighbour(down_ref, k)], axis=0)
        return jnp.where(mask > 0, joined, 0.0)

    state = [whole(f) for f in range(4)]
    damping = [whole(4 + f) for f in range(4)]
    vx, vy, b, p = state
    half = 0.5 * mask
    linear = (
        -half * rise_rows(p),
        -half * rise_columns(p) + b,
        -buoyancy_sq * vy,
        -half * (rise_rows(vx) + rise_columns(vy)),
    )
    for f in range(4):
        square = damping[f] * state[f] * state[f]
        basis_ref[0, f] = linear[f] - square * state[f]
        drag_ref[f] = (3.0 * dt_total / RADIUS) * square
    half = (0.5 * dt_total / RADIUS) * mask
    drag = [drag_ref[f] + SHIFT / RADIUS for f in range(4)]
    steps = BLOCKS[0]
    for step in range(steps):
        skip = (HALO - (KRYLOV - step)) // 8 * 8 if step else 0
        lines = slice(skip, rows - skip)
        current = [basis_ref[step, f, lines] for f in range(4)]
        for f, value in enumerate(power_step(current, [d[lines] for d in drag], half[lines])):
            basis_ref[step + 1, f, lines] = value

    def interior(j):
        return lambda: [basis_ref[j, f, HALO : rows - HALO, :width] for f in range(4)]

    gram_out([], [interior(j) for j in range(steps + 1)], table_ref, send_ref)


dot = functools.partial(jnp.dot, precision=HIGH, preferred_element_type=jnp.float32)
TILE = (SLOTS, LANES)


def tall(x):
    return jnp.concatenate([x, jnp.zeros((LANES - x.shape[0], LANES), jnp.float32)], axis=0)


def down_sum(x):
    return jnp.sum(x, axis=0, keepdims=True)


def across_sum(x):
    return jnp.sum(x, axis=1, keepdims=True)


def gram_matrix(received_ref, first, count):
    devices = received_ref.shape[0]
    row, lane = iota(TILE, 0), iota(TILE, 1)
    parts = []
    for packed in tree_sum([(received_ref[d : d + 8, 0, :], received_ref[d : d + 8, 1, :]) for d in range(0, devices, 8)]):
        packed = jnp.concatenate([packed, packed], axis=0)
        below = jnp.zeros(TILE, jnp.float32)
        for j in range(count + 1):
            line = pltpu.roll(packed, LANES - j * SLOTS, 1) if j else packed
            below = jnp.where((row == first + j) & (lane < SLOTS), line, below)
        parts.append(jnp.where(row >= first, below, jnp.where(lane >= first, flip(below), 0.0)))
    return parts[0] + old_unit(first), parts[1]


def old_unit(first):
    row, lane = iota(TILE, 0), iota(TILE, 1)
    return jnp.where((row == lane) & (row < first), 1.0, 0.0)


def flip(x):
    return jnp.transpose(tall(x))[:SLOTS]


def small_dot(a, b):
    terms = [a[:, k : k + 1] * b[k : k + 1] for k in range(KRYLOV + 1)]
    while len(terms) > 1:
        terms = [terms[k] + terms[k + 1] for k in range(0, len(terms) - 1, 2)] + terms[len(terms) // 2 * 2 :]
    return terms[0]


def gram_schmidt(gram, steps, start, hess, first, count):
    row, lane = iota(TILE, 0), iota(TILE, 1)
    unit = jnp.where(row == lane, 1.0, 0.0)
    turned = flip(steps)
    pull = small_dot(gram, turned)
    scale = jnp.where(row == first, start, jnp.where(row < first, 1.0, 0.0))
    coefs = unit * scale
    tests = pull * scale
    products = across_sum(tests * jnp.where(lane[0:1] == first, start, 0.0))
    z = down_sum(steps * jnp.where(row[:, 0:1] == first, start, 0.0)) - down_sum(coefs * products)
    for c in range(first, first + count):
        column, image = across_sum(unit * z), across_sum(gram * z)
        square = jnp.maximum(down_sum(column * image), 0.0) + norm_eps
        inverse = lax.rsqrt(square)
        inverse = inverse * (1.5 - 0.5 * square * inverse * inverse)
        hess_row = down_sum(unit * products) + jnp.where(lane[0:1] == c + 1, square * inverse, 0.0)
        hess = jnp.where(row == c, hess_row, hess)
        coefs = jnp.where(row == c + 1, z * inverse, coefs)
        if c + 1 < first + count:
            moved, older = across_sum(turned * z), across_sum(tests * z)
            own = down_sum(image * moved) * inverse * inverse
            products = older * inverse + jnp.where(row[:, 0:1] == c + 1, own, 0.0)
            tests = jnp.where(row == c + 1, down_sum(pull * column) * inverse, tests)
            z = down_sum(steps * column) * inverse - down_sum(coefs * products)
    return coefs, hess


def refined_gram(coefs, gram, gram_low, first, count):
    row, lane = iota(TILE, 0), iota(TILE, 1)
    slots = range(first + count + 1)
    gram_parts = split(gram)
    zero = jnp.zeros(TILE, jnp.float32)
    image = (zero, zero)
    for j in slots:
        line = slice(j, j + 1)
        column = coefs[:, line]
        image = add_product(image, column, gram[line], [part[line] for part in gram_parts])
        image = image[0], image[1] + column * gram_low[line]
    turned = flip(coefs)
    turned_parts = split(turned)
    result = (zero, zero)
    for i in slots:
        line = slice(i, i + 1)
        result = add_product(result, image[0][:, line], turned[line], [part[line] for part in turned_parts])
        result = result[0], result[1] + image[1][:, line] * turned[line]
    inner = (row < first) & (lane < first)
    return jnp.where(inner, old_unit(first), result[0] + result[1])


def basis_terms(hess, first):
    if first == 0:
        return jnp.full((1, 1), SHIFT, jnp.float32), jnp.zeros((1, 1), jnp.float32)
    c = first - 1
    shift = 0.5 * (hess[c - 1 : c, c - 1 : c] + hess[c : c + 1, c : c + 1])
    return shift, hess[c : c + 1, c - 1 : c]


def orthogonalize(received_ref, hess, first, count):
    gram, gram_low = gram_matrix(received_ref, first, count)
    row, lane = iota(TILE, 0), iota(TILE, 1)
    shift, back = basis_terms(hess, first)
    fresh = (row >= first) & (row < first + count)
    chain = jnp.where(lane == row, shift, 0.0) + jnp.where(lane == row + 1, RADIUS, 0.0)
    chain = chain + jnp.where((lane == row - 1) & (row > first), back, 0.0)
    steps = hess + jnp.where(fresh, chain, 0.0)
    one = jnp.ones((1, 1), jnp.float32)
    beta = jnp.sqrt(gram[0:1, 0:1] + norm_eps)
    coefs, image = gram_schmidt(gram, steps, one if first else 1.0 / beta, hess, first, count)
    if first:
        return coefs, image, beta
    gram = refined_gram(coefs, gram, gram_low, first, count)
    again, hess = gram_schmidt(gram, image, one, hess, first, count)
    return small_dot(again, coefs), hess, beta


def combine(coefs, c, parts):
    total = None
    for i, part in parts:
        term = coefs[c : c + 1, i : i + 1] * part()
        total = term if total is None else total + term
    return total


def middle_kernel(received_ref, drag_in_ref, basis_in_ref, basis_ref, kept_ref, small_ref, send_ref, table_ref):
    first, count = BLOCKS
    rows, columns = basis_ref.shape[2:]
    edge = (basis_in_ref.shape[2] - rows) // 2
    halo = HALO - edge
    body = columns - LANES
    coefs, hess, beta = orthogonalize(received_ref, jnp.zeros(TILE, jnp.float32), 0, first)
    small_ref[0] = hess
    small_ref[1] = jnp.broadcast_to(beta, TILE)
    for f in range(4):
        inner = [(j, lambda j=j: basis_in_ref[j, f, HALO : edge + rows - halo, :body]) for j in range(first + 1)]
        for c in range(first):
            kept_ref[c, f] = combine(coefs, c, inner[: c + 1])
        outer = [(j, lambda j=j: basis_in_ref[j, f, edge : edge + rows]) for j in range(first + 1)]
        basis_ref[0, f] = combine(coefs, first, outer)
    shift, back = basis_terms(hess, first)
    back = back * (1.0 / RADIUS)
    half = (0.5 * dt_total / RADIUS) * grid_mask(rows, columns, halo)
    drag = [drag_in_ref[f, edge : edge + rows] + shift * (1.0 / RADIUS) for f in range(4)]
    for step in range(count):
        current = [basis_ref[step, f] for f in range(4)]
        for f, value in enumerate(power_step(current, drag, half)):
            basis_ref[step + 1, f] = value - back * basis_ref[step - 1, f] if step else value

    def interior(ref, j, lines):
        return lambda: [ref[j, f, lines, :body] for f in range(4)]

    gram_out(
        [interior(kept_ref, i, slice(None)) for i in range(first)],
        [interior(basis_ref, j, slice(halo, rows - halo)) for j in range(count + 1)],
        table_ref,
        send_ref,
    )


def block_parts(kept_ref, basis_ref, f):
    first, count = BLOCKS
    height, body = kept_ref.shape[2:]
    halo = (basis_ref.shape[2] - height) // 2
    parts = [(i, lambda i=i: kept_ref[i, f]) for i in range(first)]
    return parts + [(first + j, lambda j=j: basis_ref[j, f, halo : halo + height, :body]) for j in range(count + 1)]


def last_kernel(received_ref, small_ref, kept_ref, basis_ref, small_out_ref, peak_ref):
    coefs, hess, _ = orthogonalize(received_ref, small_ref[0], *BLOCKS)
    small_out_ref[0] = hess
    small_out_ref[1] = small_ref[1]
    small_out_ref[2] = coefs
    for f in range(4):
        peak = jnp.max(jnp.abs(combine(coefs, KRYLOV, block_parts(kept_ref, basis_ref, f))), axis=0, keepdims=True)
        for d in range(peak_ref.shape[0]):
            peak_ref[d, f : f + 1] = peak


def exp_kernel(weights_ref, small_ref, state_ref, kept_ref, basis_ref, combined_ref, highest_ref):
    hess, beta, coefs = small_ref[0], small_ref[1, 0:1, 0:1], small_ref[2]
    size = SUBSTEPS * SLOTS
    row, lane = iota((size, LANES), 0), iota((size, LANES), 1)
    row_in, lane_in = row % SLOTS, lane % SLOTS
    same = (row // SLOTS == lane // SLOTS) & (lane < size)
    lower = jnp.where((row_in < KRYLOV) & (lane < KRYLOV), jnp.concatenate([hess] * SUBSTEPS, axis=0), 0.0)
    wide = lower
    for k in range(1, SUBSTEPS):
        wide = jnp.where(lane // SLOTS == k, pltpu.roll(lower, k * SLOTS, 1), wide)
    fraction = ((row // SLOTS) + 1).astype(jnp.float32) * (1.0 / SUBSTEPS)
    scaled = jnp.where(same, wide * fraction, 0.0)
    scaled = scaled + jnp.where(same & (row_in == KRYLOV) & (lane_in == 0), 1.0, 0.0)
    scaled = scaled * (1.0 / 2.0**squarings)
    unit = jnp.where(row == lane, 1.0, 0.0)

    def times(a, b):
        return dot(a, tall(b))

    power = [unit, scaled, times(scaled, scaled)]
    power += [times(power[2], scaled), times(power[2], power[2])]

    def group(k, count):
        total = None
        for i in range(count):
            term = power[i] * (1.0 / math.factorial(k + i))
            total = term if total is None else total + term
        return total

    top = taylor_degree - 4
    result = group(top, 5)
    while top > 0:
        top -= 4
        result = times(result, power[4]) + group(top, 4)
    for _ in range(squarings):
        result = times(result, result)
    mixing = jnp.zeros((1, LANES), jnp.float32)
    highest = jnp.zeros((1, 1), jnp.float32)
    for k in range(SUBSTEPS):
        tau = (k + 1) / SUBSTEPS
        factor = dt_total * tau
        g = result[k * SLOTS + KRYLOV : k * SLOTS + KRYLOV + 1, :]
        g = pltpu.roll(g, LANES - k * SLOTS, 1) if k else g
        mixing = mixing + weights_ref[k] * factor * beta * g
        estimate = (factor * tau) * beta * hess[KRYLOV - 1 : KRYLOV, KRYLOV : KRYLOV + 1] * jnp.abs(g[:, KRYLOV - 1 : KRYLOV])
        highest = jnp.maximum(highest, estimate)
    mixing = jnp.where(lane[0:8] < KRYLOV, jnp.broadcast_to(mixing, (8, LANES)), 0.0)
    share = dot(mixing, tall(coefs))
    for f in range(4):
        combined_ref[f] = state_ref[f] + combine(share, 0, block_parts(kept_ref, basis_ref, f))
    highest_ref[...] = jnp.broadcast_to(highest, highest_ref.shape)


def finish_kernel(highest_ref, peaks_ref, error_ref):
    error_ref[...] = jnp.max(peaks_ref[...], axis=0) * highest_ref[0:1, 0:1]


def shards(state, damping, weights):
    fields, height, width = state.shape
    columns = width + LANES
    lines = lax.axis_size("sub") * lax.axis_size("gx")
    sides = lax.axis_size("gy")
    devices = lines * sides
    f32 = lambda *shape: jax.ShapeDtypeStruct(shape, jnp.float32)
    near = lambda *shape: pltpu.VMEM(shape, jnp.float32)

    def call(kernel, outs, *args, smem=(), far=(), scratch=()):
        space = lambda k: pltpu.SMEM if k in smem else pltpu.HBM if k in far else pltpu.VMEM
        specs = [pl.BlockSpec(memory_space=space(k)) for k in range(len(args))]
        args = [a if k in smem else pltpu.with_memory_space_constraint(a, space(k)) for k, a in enumerate(args)]
        return pl.pallas_call(
            kernel,
            out_shape=outs,
            in_specs=specs,
            out_specs=[VMEM] * len(outs),
            scratch_shapes=list(scratch),
            compiler_params=pltpu.CompilerParams(vmem_limit_bytes=16 * 2**20),
        )(*args)

    exchange = lambda x, axes: lax.all_to_all(x, axes, 0, 0)
    table = near(LANES, LANES)
    send_shape = near(devices, 2, LANES)
    short = height + HALO
    first, count = BLOCKS

    whole = near(fields, height, width)
    state, damping, *edges = call(
        edge_kernel,
        [whole, whole] + [near(height, LANES)] * (1 if sides == 2 else 2),
        state,
        damping,
        far=(0, 1),
        scratch=[pltpu.SemaphoreType.DMA((2,))],
    )
    if sides == 2:
        halos = [lax.ppermute(edges[0], "gy", [(0, 1), (1, 0)])]
    else:
        halos = [
            lax.ppermute(edges[0], "gy", [((i + 1) % sides, i) for i in range(sides)]),
            lax.ppermute(edges[1], "gy", [(i, (i + 1) % sides) for i in range(sides)]),
        ]
    number = len(halos)
    stack = (8 * (width // LANES) + number) * HALO
    packs = call(
        functools.partial(pack_kernel, number),
        [near(stack, LANES)] * (1 if height == HALO else 2),
        state,
        damping,
        *halos,
    )
    up = lax.ppermute(packs[0], ROWS, [(i, (i + 1) % lines) for i in range(lines)])
    down = lax.ppermute(packs[-1], ROWS, [((i + 1) % lines, i) for i in range(lines)])
    tall_rows = height + 2 * HALO
    basis, drag, send = call(
        functools.partial(first_kernel, number),
        [near(first + 1, fields, tall_rows, columns), near(fields, tall_rows, columns), send_shape],
        state,
        damping,
        *halos,
        up,
        down,
        scratch=[table],
    )
    basis, kept, small, send = call(
        middle_kernel,
        [near(count + 1, fields, short, columns), near(first, fields, height, width), near(2, *TILE), send_shape],
        exchange(send, ALL),
        drag,
        basis,
        scratch=[table],
    )
    small, peaks = call(
        last_kernel,
        [near(3, *TILE), near(lines, fields, width)],
        exchange(send, ALL),
        small,
        kept,
        basis,
    )
    combined, highest = call(
        exp_kernel,
        [f32(fields, height, width), near(8, LANES)],
        weights,
        small,
        state,
        kept,
        basis,
        smem=(0,),
    )
    (column_error,) = call(finish_kernel, [f32(fields, width)], highest, exchange(peaks, ROWS))
    return combined, column_error


def solution(mesh):
    return jax.shard_map(
        shards,
        mesh=mesh,
        in_specs=(P(None, ROWS, "gy"), P(None, ROWS, "gy"), P()),
        out_specs=(P(None, ROWS, "gy"), P(None, "gy")),
        check_vma=False,
    )
```

```python
import functools
import math

import jax
import jax.numpy as jnp
from jax import lax
from jax.experimental import pallas as pl
from jax.experimental.pallas import tpu as pltpu
from jax.sharding import PartitionSpec as P

KRYLOV = 12
SUBSTEPS = 4
BLOCKS = (6, 6)
HALO = 16
LANES = 128
SLOTS = 16
EDGE = 16

dt_total = 4.0
buoyancy_sq = 0.5
norm_eps = 1e-06
taylor_degree = 12
squarings = 8
SHIFT = -2.0
RADIUS = 4.0

ROWS = ("sub", "gx")
ALL = ("sub", "gx", "gy")
HIGH = lax.Precision.HIGHEST
VMEM = pl.BlockSpec(memory_space=pltpu.VMEM)


def iota(shape, dim):
    return lax.broadcasted_iota(jnp.int32, shape, dim)


def rise_rows(x):
    return pltpu.roll(x, x.shape[0] - 1, 0) - pltpu.roll(x, 1, 0)


def rise_columns(x):
    return pltpu.roll(x, x.shape[1] - 1, 1) - pltpu.roll(x, 1, 1)


def grid_mask(rows, columns, halo_rows):
    line, lane = iota((rows, columns), 0), iota((rows, columns), 1)
    place = lax.axis_index("sub") * lax.axis_size("gx") + lax.axis_index("gx")
    last = lax.axis_size("sub") * lax.axis_size("gx") - 1
    side = lax.axis_index("gy")
    first_line = jnp.where(place > 0, 0, halo_rows)
    end_line = jnp.where(place < last, rows, rows - halo_rows)
    body = columns - LANES
    right_end = jnp.where(side < lax.axis_size("gy") - 1, body + EDGE, body)
    left_start = jnp.where(side > 0, columns - EDGE, columns)
    inside = (line >= first_line) & (line < end_line) & ((lane < right_end) | (lane >= left_start))
    return jnp.where(inside, 1.0, 0.0)


def power_step(fields, drag, half):
    vx, vy, b, p = fields
    quarter = dt_total / RADIUS
    return (
        -half * rise_rows(p) - drag[0] * vx,
        -half * rise_columns(p) + quarter * b - drag[1] * vy,
        (-buoyancy_sq * quarter) * vy - drag[2] * b,
        -half * (rise_rows(vx) + rise_columns(vy)) - drag[3] * p,
    )


def two_sum(a, b):
    total = a + b
    part = total - a
    return total, (a - (total - part)) + (b - part)


def pair_sum(one, two):
    total, error = two_sum(one[0], two[0])
    return total, one[1] + two[1] + error


def split(a):
    scaled = 4097.0 * a
    high = scaled - (scaled - a)
    return high, a - high


def add_product(total, a, b, b_parts):
    product = a * b
    a_high, a_low = split(a)
    error = ((a_high * b_parts[0] - product) + a_high * b_parts[1] + a_low * b_parts[0]) + a_low * b_parts[1]
    high, rest = two_sum(total[0], product)
    return high, total[1] + (rest + error)


def tree_sum(tiles):
    while len(tiles) > 1:
        tiles = [pair_sum(tiles[k], tiles[k + 1]) for k in range(0, len(tiles) - 1, 2)] + tiles[len(tiles) // 2 * 2 :]
    total = tiles[0]
    for shift in (4, 2, 1):
        total = pair_sum(total, (pltpu.roll(total[0], shift, 0), pltpu.roll(total[1], shift, 0)))
    return total


def pair_rows(one, two):
    total = None
    for f in range(4):
        prod = one[f] * two[f]
        part = None
        for r in range(0, prod.shape[0], 8):
            for c in range(0, prod.shape[1], LANES):
                tile = prod[r : r + 8, c : c + LANES]
                part = tile if part is None else part + tile
        total = part if total is None else total + part
    return jnp.sum(total, axis=0, keepdims=True)


def gram_out(old, new, table_ref, send_ref):
    first = len(old)
    table_ref[...] = jnp.zeros_like(table_ref)
    for j in range(len(new)):
        for i in range(first):
            table_ref[j * SLOTS + i : j * SLOTS + i + 1, :] = pair_rows(old[i](), new[j]())
        for i in range(j + 1):
            row = pair_rows(new[i](), new[j]())
            table_ref[j * SLOTS + first + i : j * SLOTS + first + i + 1, :] = row
            if i != j:
                table_ref[i * SLOTS + first + j : i * SLOTS + first + j + 1, :] = row
    turned = jnp.transpose(table_ref[...])
    zero = jnp.zeros((8, LANES), jnp.float32)
    high, low = tree_sum([(turned[r : r + 8], zero) for r in range(0, LANES, 8)])
    for d in range(send_ref.shape[0]):
        send_ref[d, 0:1] = high[0:1]
        send_ref[d, 1:2] = low[0:1]


def edge_kernel(far_state_ref, far_damping_ref, state_ref, damping_ref, *refs):
    edge_refs, semaphores = refs[:-1], refs[-1]
    copies = [
        pltpu.make_async_copy(far_state_ref, state_ref, semaphores.at[0]),
        pltpu.make_async_copy(far_damping_ref, damping_ref, semaphores.at[1]),
    ]
    for copy in copies:
        copy.start()
    for copy in copies:
        copy.wait()
    width = state_ref.shape[2]
    lane = iota((state_ref.shape[1], LANES), 1)

    def packed(pick):
        total = None
        for k in range(8):
            ref = state_ref if k < 4 else damping_ref
            head, tail = ref[k % 4, :, :LANES], ref[k % 4, :, width - LANES :]
            tile = pltpu.roll(pick(head, pltpu.roll(tail, EDGE, 1)), k * EDGE, 1) if k else pick(head, pltpu.roll(tail, EDGE, 1))
            total = tile if total is None else jnp.where(lane // EDGE == k, tile, total)
        return total

    if len(edge_refs) == 1:
        left = lax.axis_index("gy") == 0
        edge_refs[0][...] = packed(lambda head, tail: jnp.where(left, tail, head))
    else:
        edge_refs[0][...] = packed(lambda head, tail: head)
        edge_refs[1][...] = packed(lambda head, tail: tail)


def pack_kernel(count, state_ref, damping_ref, *refs):
    halo_refs, out_refs = refs[:count], refs[count:]
    height, width = state_ref.shape[1:]
    for out_ref, start in zip(out_refs, (height - HALO, 0)):
        lines = slice(start, start + HALO)
        at = 0
        for k in range(8):
            ref = state_ref if k < 4 else damping_ref
            for c in range(0, width, LANES):
                out_ref[at : at + HALO] = ref[k % 4, lines, c : c + LANES]
                at += HALO
        for halo_ref in halo_refs:
            out_ref[at : at + HALO] = halo_ref[lines]
            at += HALO


def first_kernel(count, state_ref, damping_ref, *refs):
    halo_refs = refs[:count]
    up_ref, down_ref, basis_ref, drag_ref, send_ref, table_ref = refs[count:]
    height, width = state_ref.shape[1:]
    rows, columns = height + 2 * HALO, width + LANES
    tiles = width // LANES
    mask = grid_mask(rows, columns, HALO)

    def side_tile(k, right, left):
        lane = iota(right.shape, 1)
        right = pltpu.roll(right, LANES - k * EDGE, 1) if k else right
        return jnp.where(lane < LANES // 2, right, pltpu.roll(left, LANES - (k + 1) * EDGE, 1) if k < 7 else left)

    def neighbour(ref, k):
        parts = [ref[(k * tiles + t) * HALO : (k * tiles + t + 1) * HALO] for t in range(tiles)]
        at = 8 * tiles * HALO
        ends = [ref[at + c * HALO : at + (c + 1) * HALO] for c in range(count)]
        return jnp.concatenate(parts + [side_tile(k, ends[0], ends[-1])], axis=1)

    def whole(k):
        ref = state_ref if k < 4 else damping_ref
        own = jnp.concatenate([ref[k % 4], side_tile(k, halo_refs[0][...], halo_refs[-1][...])], axis=1)
        joined = jnp.concatenate([neighbour(up_ref, k), own, neighbour(down_ref, k)], axis=0)
        return jnp.where(mask > 0, joined, 0.0)

    state = [whole(f) for f in range(4)]
    damping = [whole(4 + f) for f in range(4)]
    vx, vy, b, p = state
    half = 0.5 * mask
    linear = (
        -half * rise_rows(p),
        -half * rise_columns(p) + b,
        -buoyancy_sq * vy,
        -half * (rise_rows(vx) + rise_columns(vy)),
    )
    for f in range(4):
        square = damping[f] * state[f] * state[f]
        basis_ref[0, f] = linear[f] - square * state[f]
        drag_ref[f] = (3.0 * dt_total / RADIUS) * square
    half = (0.5 * dt_total / RADIUS) * mask
    drag = [drag_ref[f] + SHIFT / RADIUS for f in range(4)]
    steps = BLOCKS[0]
    for step in range(steps):
        skip = (HALO - (KRYLOV - step)) // 8 * 8 if step else 0
        lines = slice(skip, rows - skip)
        current = [basis_ref[step, f, lines] for f in range(4)]
        for f, value in enumerate(power_step(current, [d[lines] for d in drag], half[lines])):
            basis_ref[step + 1, f, lines] = value

    def interior(j):
        return lambda: [basis_ref[j, f, HALO : rows - HALO, :width] for f in range(4)]

    gram_out([], [interior(j) for j in range(steps + 1)], table_ref, send_ref)


dot = functools.partial(jnp.dot, precision=HIGH, preferred_element_type=jnp.float32)
TILE = (SLOTS, LANES)


def block_tile(first, count):
    return (-(-(first + count + 1) // 8) * 8, LANES)


def tall(x):
    return jnp.concatenate([x, jnp.zeros((LANES - x.shape[0], LANES), jnp.float32)], axis=0)


def down_sum(x):
    return jnp.sum(x, axis=0, keepdims=True)


def across_sum(x):
    return jnp.sum(x, axis=1, keepdims=True)


def gram_matrix(received_ref, first, count):
    devices = received_ref.shape[0]
    tile = block_tile(first, count)
    row, lane = iota(tile, 0), iota(tile, 1)
    parts = []
    for packed in tree_sum([(received_ref[d : d + 8, 0, :], received_ref[d : d + 8, 1, :]) for d in range(0, devices, 8)]):
        packed = jnp.concatenate([packed] * (tile[0] // 8), axis=0)
        below = jnp.zeros(tile, jnp.float32)
        for j in range(count + 1):
            line = pltpu.roll(packed, LANES - j * SLOTS, 1) if j else packed
            below = jnp.where((row == first + j) & (lane < SLOTS), line, below)
        parts.append(jnp.where(row >= first, below, jnp.where(lane >= first, flip(below), 0.0)))
    return parts[0] + old_unit(first, tile), parts[1]


def old_unit(first, tile):
    row, lane = iota(tile, 0), iota(tile, 1)
    return jnp.where((row == lane) & (row < first), 1.0, 0.0)


def flip(x):
    return jnp.transpose(tall(x))[: x.shape[0]]


def added(terms):
    while len(terms) > 1:
        terms = [terms[k] + terms[k + 1] for k in range(0, len(terms) - 1, 2)] + terms[len(terms) // 2 * 2 :]
    return terms[0]


def columns_of(matrix, count):
    return [jnp.broadcast_to(matrix[:, a : a + 1], matrix.shape) for a in range(count)]


def weighted(columns, x):
    return added([x[a : a + 1] * column for a, column in enumerate(columns)])


def gram_matrix(received_ref, first, count):
    devices = received_ref.shape[0]
    tile = block_tile(first, count)
    row, lane = iota(tile, 0), iota(tile, 1)
    parts = []
    for packed in tree_sum([(received_ref[d : d + 8, 0, :], received_ref[d : d + 8, 1, :]) for d in range(0, devices, 8)]):
        packed = jnp.concatenate([packed] * (tile[0] // 8), axis=0)
        below = jnp.zeros(tile, jnp.float32)
        for j in range(count + 1):
            line = pltpu.roll(packed, LANES - j * SLOTS, 1) if j else packed
            below = jnp.where((row == first + j) & (lane < SLOTS), line, below)
        parts.append(jnp.where(row >= first, below, jnp.where(lane >= first, flip(below), 0.0)))
    return parts[0] + old_unit(first, tile), parts[1]


def old_unit(first, tile):
    row, lane = iota(tile, 0), iota(tile, 1)
    return jnp.where((row == lane) & (row < first), 1.0, 0.0)


def flip(x):
    return jnp.transpose(tall(x))[: x.shape[0]]


def small_dot(a, b):
    terms = [a[:, k : k + 1] * b[k : k + 1] for k in range(min(KRYLOV + 1, b.shape[0]))]
    while len(terms) > 1:
        terms = [terms[k] + terms[k + 1] for k in range(0, len(terms) - 1, 2)] + terms[len(terms) // 2 * 2 :]
    return terms[0]


def gram_schmidt(gram, image_of, start, first, count):
    row = iota(gram[0].shape, 0)
    vector = jnp.where(row == first, start, 0.0)
    raw, raw_image, inverse = vector, gram[first] * start, 1.0
    vectors, images, hess = [vector], [], []
    for c in range(first, first + count):
        moved = image_of(raw, c)
        products = [down_sum(image * moved) for image in images]
        own = down_sum(raw_image * moved) * (inverse * inverse)
        images.append(raw_image * inverse)
        rest = added([moved] + [-product * other for product, other in zip(products, vectors)])
        seen = added([jnp.where(row == first + k, product, 0.0) for k, product in enumerate(products)] + [jnp.zeros_like(moved)])
        if first:
            older = jnp.where(row < first, weighted(gram[: c + 2], moved), 0.0)
            rest, seen = rest - older, seen + older
        raw = rest * inverse - own * vectors[-1]
        column = seen * inverse + jnp.where(row == c, own, 0.0)
        raw_image = weighted(gram[: c + 2], raw)
        square = jnp.maximum(down_sum(raw * raw_image), 0.0) + norm_eps
        inverse = lax.rsqrt(square)
        inverse = inverse * (1.5 - 0.5 * square * inverse * inverse)
        vectors.append(raw * inverse)
        hess.append(column + jnp.where(row == c + 1, square * inverse, 0.0))
    return vectors, hess


def by_lane(columns, first, matrix):
    lane = iota(matrix.shape, 1)
    for k, column in enumerate(columns):
        matrix = jnp.where(lane == first + k, column, matrix)
    return matrix


def refined_gram(vectors, gram, gram_low):
    row = iota(gram[0].shape, 0)
    zero = jnp.zeros_like(gram[0])
    turned = by_lane(vectors, 0, zero)
    parts = split(turned)
    image = (zero, zero)
    for j, (column, low) in enumerate(zip(gram, gram_low)):
        line = slice(j, j + 1)
        image = add_product(image, column, turned[line], [part[line] for part in parts])
        image = image[0], image[1] + low * turned[line]
    image_parts = split(image[0])
    result = zero
    for c, vector in enumerate(vectors):
        high, low = add_product((zero, zero), vector, image[0], image_parts)
        high, low = tree_sum([(high, low + vector * image[1])])
        result = jnp.where(row == c, high + low, result)
    return result


def basis_terms(hess, first):
    c = first - 1
    shift = 0.5 * (hess[c - 1][c - 1 : c] + hess[c][c : c + 1])
    return shift, hess[c][c - 1 : c]


def orthogonalize(received_ref, hess, first, count):
    gram, gram_low = gram_matrix(received_ref, first, count)
    slots = first + count + 1
    gram = columns_of(gram, slots)
    row = iota(gram[0].shape, 0)

    def basis_image(x, c):
        fresh = jnp.where(row >= first, x, 0.0)
        if not first:
            return RADIUS * pltpu.roll(fresh, 1, 0) + SHIFT * fresh
        shift, back = basis_terms(hess, first)
        image = RADIUS * pltpu.roll(fresh, 1, 0) + shift * fresh
        image = image + jnp.where(row >= first, back * pltpu.roll(fresh, row.shape[0] - 1, 0), 0.0)
        return image + weighted(hess, x)

    if first:
        return *gram_schmidt(gram, basis_image, 1.0, first, count), None
    square = gram[0][0:1] + norm_eps
    beta = jnp.sqrt(square)
    vectors, image = gram_schmidt(gram, basis_image, 1.0 / beta, first, count)
    gram = columns_of(refined_gram(vectors, gram, columns_of(gram_low, slots)), slots)
    again, hess = gram_schmidt(gram, lambda x, c: weighted(image[: c + 1], x), 1.0, first, count)
    return [weighted(vectors[: c + 1], x) for c, x in enumerate(again)], hess, beta


def combine(weights, parts):
    total = None
    for i, part in parts:
        value = part()
        scale = jnp.concatenate([weights[i : i + 1]] * (value.shape[1] // LANES), axis=1)
        total = scale * value if total is None else total + scale * value
    return total


def middle_kernel(received_ref, drag_in_ref, basis_in_ref, basis_ref, kept_ref, small_ref, send_ref, table_ref):
    first, count = BLOCKS
    rows, columns = basis_ref.shape[2:]
    edge = (basis_in_ref.shape[2] - rows) // 2
    halo = HALO - edge
    body = columns - LANES
    vectors, hess, beta = orthogonalize(received_ref, [], 0, first)
    small_ref[0] = jnp.zeros(TILE, jnp.float32)
    small_ref[0, : hess[0].shape[0]] = by_lane(hess, 0, jnp.zeros_like(hess[0]))
    small_ref[1] = jnp.broadcast_to(beta, TILE)
    for f in range(4):
        inner = [(j, lambda j=j: basis_in_ref[j, f, HALO : edge + rows - halo, :body]) for j in range(first + 1)]
        for c in range(first):
            kept_ref[c, f] = combine(vectors[c], inner[: c + 1])
        outer = [(j, lambda j=j: basis_in_ref[j, f, edge : edge + rows]) for j in range(first + 1)]
        basis_ref[0, f] = combine(vectors[first], outer)
    wide = lambda x: jnp.concatenate([x * (1.0 / RADIUS)] * (columns // LANES), axis=1)
    shift, back = map(wide, basis_terms(hess, first))
    half = (0.5 * dt_total / RADIUS) * grid_mask(rows, columns, halo)
    drag = [drag_in_ref[f, edge : edge + rows] + shift for f in range(4)]
    for step in range(count):
        current = [basis_ref[step, f] for f in range(4)]
        for f, value in enumerate(power_step(current, drag, half)):
            basis_ref[step + 1, f] = value - back * basis_ref[step - 1, f] if step else value

    def interior(ref, j, lines):
        return lambda: [ref[j, f, lines, :body] for f in range(4)]

    gram_out(
        [interior(kept_ref, i, slice(None)) for i in range(first)],
        [interior(basis_ref, j, slice(halo, rows - halo)) for j in range(count + 1)],
        table_ref,
        send_ref,
    )


def block_parts(kept_ref, basis_ref, f):
    first, count = BLOCKS
    height, body = kept_ref.shape[2:]
    halo = (basis_ref.shape[2] - height) // 2
    parts = [(i, lambda i=i: kept_ref[i, f]) for i in range(first)]
    return parts + [(first + j, lambda j=j: basis_ref[j, f, halo : halo + height, :body]) for j in range(count + 1)]


def last_kernel(received_ref, small_ref, kept_ref, basis_ref, small_out_ref, peak_ref):
    first, count = BLOCKS
    old = small_ref[0]
    vectors, hess, _ = orthogonalize(received_ref, columns_of(old, first), first, count)
    small_out_ref[0] = by_lane(hess, first, old)
    small_out_ref[1] = small_ref[1]
    small_out_ref[2] = by_lane(vectors, first, old_unit(first, TILE))
    for f in range(4):
        peak = jnp.max(jnp.abs(combine(vectors[count], block_parts(kept_ref, basis_ref, f))), axis=0, keepdims=True)
        for d in range(peak_ref.shape[0]):
            peak_ref[d, f : f + 1] = peak


def exp_kernel(weights_ref, small_ref, state_ref, kept_ref, basis_ref, combined_ref, highest_ref):
    hess, beta, vectors = flip(small_ref[0]), small_ref[1, 0:1, 0:1], small_ref[2]
    size = SUBSTEPS * SLOTS
    row, lane = iota((size, LANES), 0), iota((size, LANES), 1)
    row_in, lane_in = row % SLOTS, lane % SLOTS
    same = (row // SLOTS == lane // SLOTS) & (lane < size)
    lower = jnp.where((row_in < KRYLOV) & (lane < KRYLOV), jnp.concatenate([hess] * SUBSTEPS, axis=0), 0.0)
    wide = lower
    for k in range(1, SUBSTEPS):
        wide = jnp.where(lane // SLOTS == k, pltpu.roll(lower, k * SLOTS, 1), wide)
    fraction = ((row // SLOTS) + 1).astype(jnp.float32) * (1.0 / SUBSTEPS)
    scaled = jnp.where(same, wide * fraction, 0.0)
    scaled = scaled + jnp.where(same & (row_in == KRYLOV) & (lane_in == 0), 1.0, 0.0)
    scaled = scaled * (1.0 / 2.0**squarings)
    unit = jnp.where(row == lane, 1.0, 0.0)

    def times(a, b):
        return dot(a, tall(b))

    power = [unit, scaled, times(scaled, scaled)]
    power += [times(power[2], scaled), times(power[2], power[2])]

    def group(k, count):
        total = None
        for i in range(count):
            term = power[i] * (1.0 / math.factorial(k + i))
            total = term if total is None else total + term
        return total

    top = taylor_degree - 4
    result = group(top, 5)
    while top > 0:
        top -= 4
        result = times(result, power[4]) + group(top, 4)
    for _ in range(squarings):
        result = times(result, result)
    mixing = jnp.zeros((1, LANES), jnp.float32)
    highest = jnp.zeros((1, 1), jnp.float32)
    for k in range(SUBSTEPS):
        tau = (k + 1) / SUBSTEPS
        factor = dt_total * tau
        g = result[k * SLOTS + KRYLOV : k * SLOTS + KRYLOV + 1, :]
        g = pltpu.roll(g, LANES - k * SLOTS, 1) if k else g
        mixing = mixing + weights_ref[k] * factor * beta * g
        estimate = (factor * tau) * beta * hess[KRYLOV - 1 : KRYLOV, KRYLOV : KRYLOV + 1] * jnp.abs(g[:, KRYLOV - 1 : KRYLOV])
        highest = jnp.maximum(highest, estimate)
    mixing = jnp.where(lane[0:1] < KRYLOV, mixing, 0.0)
    share = jnp.broadcast_to(across_sum(vectors * mixing), TILE)
    for f in range(4):
        combined_ref[f] = state_ref[f] + combine(share, block_parts(kept_ref, basis_ref, f))
    highest_ref[...] = jnp.broadcast_to(highest, highest_ref.shape)


def finish_kernel(highest_ref, peaks_ref, error_ref):
    error_ref[...] = jnp.max(peaks_ref[...], axis=0) * highest_ref[0:1, 0:1]


def shards(state, damping, weights):
    fields, height, width = state.shape
    columns = width + LANES
    lines = lax.axis_size("sub") * lax.axis_size("gx")
    sides = lax.axis_size("gy")
    devices = lines * sides
    f32 = lambda *shape: jax.ShapeDtypeStruct(shape, jnp.float32)
    near = lambda *shape: pltpu.VMEM(shape, jnp.float32)

    def call(kernel, outs, *args, smem=(), far=(), scratch=()):
        space = lambda k: pltpu.SMEM if k in smem else pltpu.HBM if k in far else pltpu.VMEM
        specs = [pl.BlockSpec(memory_space=space(k)) for k in range(len(args))]
        args = [a if k in smem else pltpu.with_memory_space_constraint(a, space(k)) for k, a in enumerate(args)]
        return pl.pallas_call(
            kernel,
            out_shape=outs,
            in_specs=specs,
            out_specs=[VMEM] * len(outs),
            scratch_shapes=list(scratch),
            compiler_params=pltpu.CompilerParams(vmem_limit_bytes=16 * 2**20),
        )(*args)

    exchange = lambda x, axes: lax.all_to_all(x, axes, 0, 0)
    table = near(LANES, LANES)
    send_shape = near(devices, 2, LANES)
    short = height + HALO
    first, count = BLOCKS

    whole = near(fields, height, width)
    state, damping, *edges = call(
        edge_kernel,
        [whole, whole] + [near(height, LANES)] * (1 if sides == 2 else 2),
        state,
        damping,
        far=(0, 1),
        scratch=[pltpu.SemaphoreType.DMA((2,))],
    )
    if sides == 2:
        halos = [lax.ppermute(edges[0], "gy", [(0, 1), (1, 0)])]
    else:
        halos = [
            lax.ppermute(edges[0], "gy", [((i + 1) % sides, i) for i in range(sides)]),
            lax.ppermute(edges[1], "gy", [(i, (i + 1) % sides) for i in range(sides)]),
        ]
    number = len(halos)
    stack = (8 * (width // LANES) + number) * HALO
    packs = call(
        functools.partial(pack_kernel, number),
        [near(stack, LANES)] * (1 if height == HALO else 2),
        state,
        damping,
        *halos,
    )
    up = lax.ppermute(packs[0], ROWS, [(i, (i + 1) % lines) for i in range(lines)])
    down = lax.ppermute(packs[-1], ROWS, [((i + 1) % lines, i) for i in range(lines)])
    tall_rows = height + 2 * HALO
    basis, drag, send = call(
        functools.partial(first_kernel, number),
        [near(first + 1, fields, tall_rows, columns), near(fields, tall_rows, columns), send_shape],
        state,
        damping,
        *halos,
        up,
        down,
        scratch=[table],
    )
    basis, kept, small, send = call(
        middle_kernel,
        [near(count + 1, fields, short, columns), near(first, fields, height, width), near(2, *TILE), send_shape],
        exchange(send, ALL),
        drag,
        basis,
        scratch=[table],
    )
    small, peaks = call(
        last_kernel,
        [near(3, *TILE), near(lines, fields, width)],
        exchange(send, ALL),
        small,
        kept,
        basis,
    )
    combined, highest = call(
        exp_kernel,
        [f32(fields, height, width), near(8, LANES)],
        weights,
        small,
        state,
        kept,
        basis,
        smem=(0,),
    )
    (column_error,) = call(finish_kernel, [f32(fields, width)], highest, exchange(peaks, ROWS))
    return combined, column_error


def solution(mesh):
    return jax.shard_map(
        shards,
        mesh=mesh,
        in_specs=(P(None, ROWS, "gy"), P(None, ROWS, "gy"), P()),
        out_specs=(P(None, ROWS, "gy"), P(None, "gy")),
        check_vma=False,
    )
```

```python
import functools
import math

import jax
import jax.numpy as jnp
from jax import lax
from jax.experimental import pallas as pl
from jax.experimental.pallas import tpu as pltpu
from jax.sharding import PartitionSpec as P

KRYLOV = 12
SUBSTEPS = 4
GUESS = 6
HALO = 16
LANES = 128
SLOTS = 16
EDGE = 16

dt_total = 4.0
buoyancy_sq = 0.5
norm_eps = 1e-06
taylor_degree = 12
squarings = 8
SHIFT = -2.0
RADIUS = 4.0

ROWS = ("sub", "gx")
ALL = ("sub", "gx", "gy")
HIGH = lax.Precision.HIGHEST
VMEM = pl.BlockSpec(memory_space=pltpu.VMEM)


def iota(shape, dim):
    return lax.broadcasted_iota(jnp.int32, shape, dim)


def rise_rows(x):
    return pltpu.roll(x, x.shape[0] - 1, 0) - pltpu.roll(x, 1, 0)


def rise_columns(x):
    return pltpu.roll(x, x.shape[1] - 1, 1) - pltpu.roll(x, 1, 1)


def grid_mask(rows, columns, halo_rows):
    line, lane = iota((rows, columns), 0), iota((rows, columns), 1)
    place = lax.axis_index("sub") * lax.axis_size("gx") + lax.axis_index("gx")
    last = lax.axis_size("sub") * lax.axis_size("gx") - 1
    side = lax.axis_index("gy")
    first_line = jnp.where(place > 0, 0, halo_rows)
    end_line = jnp.where(place < last, rows, rows - halo_rows)
    body = columns - LANES
    right_end = jnp.where(side < lax.axis_size("gy") - 1, body + EDGE, body)
    left_start = jnp.where(side > 0, columns - EDGE, columns)
    inside = (line >= first_line) & (line < end_line) & ((lane < right_end) | (lane >= left_start))
    return jnp.where(inside, 1.0, 0.0)


def shifted(fields, drag, double, rows_of=rise_rows, columns_of=rise_columns):
    vx, vy, b, p = fields
    return (
        -double * rows_of(p) - drag[0] * vx,
        -double * columns_of(p) + dt_total * b - drag[1] * vy,
        (-buoyancy_sq * dt_total) * vy - drag[2] * b,
        -double * (rows_of(vx) + columns_of(vy)) - drag[3] * p,
    )


def forcing_of(state, damping, half, rows_of=rise_rows, columns_of=rise_columns):
    vx, vy, b, p = state
    linear = (
        -half * rows_of(p),
        -half * columns_of(p) + b,
        -buoyancy_sq * vy,
        -half * (rows_of(vx) + columns_of(vy)),
    )
    square = [damping[f] * state[f] * state[f] for f in range(4)]
    return [linear[f] - square[f] * state[f] for f in range(4)], [(3.0 * dt_total) * x for x in square]


def two_sum(a, b):
    total = a + b
    part = total - a
    return total, (a - (total - part)) + (b - part)


def pair_sum(one, two):
    total, error = two_sum(one[0], two[0])
    return total, one[1] + two[1] + error


def split(a):
    scaled = 4097.0 * a
    high = scaled - (scaled - a)
    return high, a - high


def add_product(total, a, b, b_parts):
    product = a * b
    a_high, a_low = split(a)
    error = ((a_high * b_parts[0] - product) + a_high * b_parts[1] + a_low * b_parts[0]) + a_low * b_parts[1]
    high, rest = two_sum(total[0], product)
    return high, total[1] + (rest + error)


def tree_sum(tiles):
    while len(tiles) > 1:
        tiles = [pair_sum(tiles[k], tiles[k + 1]) for k in range(0, len(tiles) - 1, 2)] + tiles[len(tiles) // 2 * 2 :]
    total = tiles[0]
    for shift in (4, 2, 1):
        total = pair_sum(total, (pltpu.roll(total[0], shift, 0), pltpu.roll(total[1], shift, 0)))
    return total


def pair_rows(one, two):
    total = None
    for f in range(4):
        prod = one[f] * two[f]
        part = None
        for r in range(0, prod.shape[0], 8):
            for c in range(0, prod.shape[1], LANES):
                tile = prod[r : r + 8, c : c + LANES]
                part = tile if part is None else part + tile
        total = part if total is None else total + part
    return jnp.sum(total, axis=0, keepdims=True)


GROUP = LANES // SLOTS


def gram_out(vectors, table_ref, send_ref):
    table_ref[...] = jnp.zeros_like(table_ref)
    for j in range(len(vectors)):
        for i in range(j + 1):
            table_ref[j * SLOTS + i : j * SLOTS + i + 1, :] = pair_rows(vectors[i](), vectors[j]())
    zero = jnp.zeros((8, LANES), jnp.float32)
    for g in range(table_ref.shape[0] // LANES):
        turned = jnp.transpose(table_ref[g * LANES : (g + 1) * LANES])
        high, low = tree_sum([(turned[r : r + 8], zero) for r in range(0, LANES, 8)])
        for d in range(send_ref.shape[0]):
            send_ref[d, 2 * g : 2 * g + 1] = high[0:1]
            send_ref[d, 2 * g + 1 : 2 * g + 2] = low[0:1]


def edge_kernel(far_state_ref, far_damping_ref, state_ref, damping_ref, *refs):
    edge_refs, semaphores = refs[:-1], refs[-1]
    copies = [
        pltpu.make_async_copy(far_state_ref, state_ref, semaphores.at[0]),
        pltpu.make_async_copy(far_damping_ref, damping_ref, semaphores.at[1]),
    ]
    for copy in copies:
        copy.start()
    for copy in copies:
        copy.wait()
    width = state_ref.shape[2]
    lane = iota((state_ref.shape[1], LANES), 1)

    def packed(pick):
        total = None
        for k in range(8):
            ref = state_ref if k < 4 else damping_ref
            head, tail = ref[k % 4, :, :LANES], ref[k % 4, :, width - LANES :]
            tile = pltpu.roll(pick(head, pltpu.roll(tail, EDGE, 1)), k * EDGE, 1) if k else pick(head, pltpu.roll(tail, EDGE, 1))
            total = tile if total is None else jnp.where(lane // EDGE == k, tile, total)
        return total

    if len(edge_refs) == 1:
        left = lax.axis_index("gy") == 0
        edge_refs[0][...] = packed(lambda head, tail: jnp.where(left, tail, head))
    else:
        edge_refs[0][...] = packed(lambda head, tail: head)
        edge_refs[1][...] = packed(lambda head, tail: tail)


def pack_kernel(count, state_ref, damping_ref, *refs):
    halo_refs, out_refs = refs[:count], refs[count:]
    height, width = state_ref.shape[1:]
    for out_ref, start in zip(out_refs, (height - HALO, 0)):
        lines = slice(start, start + HALO)
        at = 0
        for k in range(8):
            ref = state_ref if k < 4 else damping_ref
            for c in range(0, width, LANES):
                out_ref[at : at + HALO] = ref[k % 4, lines, c : c + LANES]
                at += HALO
        for halo_ref in halo_refs:
            out_ref[at : at + HALO] = halo_ref[lines]
            at += HALO


def first_kernel(count, state_ref, damping_ref, *refs):
    halo_refs = refs[:count]
    up_ref, down_ref, guess_ref, inner_ref, small_ref, send_ref, basis_ref, drag_ref, table_ref = refs[count:]
    height, width = state_ref.shape[1:]
    rows, columns = height + 2 * HALO, width + LANES
    tiles = width // LANES
    mask = grid_mask(rows, columns, HALO)

    def side_tile(k, right, left):
        lane = iota(right.shape, 1)
        right = pltpu.roll(right, LANES - k * EDGE, 1) if k else right
        return jnp.where(lane < LANES // 2, right, pltpu.roll(left, LANES - (k + 1) * EDGE, 1) if k < 7 else left)

    def neighbour(ref, k):
        parts = [ref[(k * tiles + t) * HALO : (k * tiles + t + 1) * HALO] for t in range(tiles)]
        at = 8 * tiles * HALO
        ends = [ref[at + c * HALO : at + (c + 1) * HALO] for c in range(count)]
        return jnp.concatenate(parts + [side_tile(k, ends[0], ends[-1])], axis=1)

    def whole(k):
        ref = state_ref if k < 4 else damping_ref
        own = jnp.concatenate([ref[k % 4], side_tile(k, halo_refs[0][...], halo_refs[-1][...])], axis=1)
        joined = jnp.concatenate([neighbour(up_ref, k), own, neighbour(down_ref, k)], axis=0)
        return jnp.where(mask > 0, joined, 0.0)

    state = [whole(f) for f in range(4)]
    damping = [whole(4 + f) for f in range(4)]
    forcing, drag = forcing_of(state, damping, 0.5 * mask)
    guess, scale = guessed(guess_ref)
    steps = basis_columns(guess)
    small_ref[0] = by_lane(steps, 0, jnp.zeros(TILE, jnp.float32))
    small_ref[1] = jnp.broadcast_to(scale, TILE)
    wide = lambda x: jnp.concatenate([x] * (columns // LANES), axis=1)
    start = wide(1.0 / scale)
    for f in range(4):
        basis_ref[0, f] = forcing[f] * start
        drag_ref[f] = drag[f]
    double = (0.5 * dt_total) * mask
    for c, column in enumerate(steps):
        skip = (HALO - (KRYLOV - c)) // 8 * 8 if c else 0
        lines = slice(skip, rows - skip)
        entry = lambda i: wide(column[i : i + 1])
        shift, inverse = entry(c), wide(1.0 / column[c + 1 : c + 2])
        current = [basis_ref[c, f, lines] for f in range(4)]
        image = shifted(current, [drag_ref[f, lines] + shift for f in range(4)], double[lines])
        for f in range(4):
            value = image[f]
            for i in range(0 if c < GUESS else c - 1, c):
                value = value - entry(i) * basis_ref[i, f, lines]
            basis_ref[c + 1, f, lines] = value * inverse

    for j in range(KRYLOV + 1):
        for f in range(4):
            inner_ref[j, f] = basis_ref[j, f, HALO : rows - HALO, :width]
    gram_out([lambda j=j: [inner_ref[j, f] for f in range(4)] for j in range(KRYLOV + 1)], table_ref, send_ref)


def guess_kernel(state_ref, damping_ref, send_ref, basis_ref, table_ref):
    height, width = state_ref.shape[1:]
    line, lane = iota((height, width), 0), iota((height, width), 1)

    def rows_of(x):
        return jnp.where(line < height - 1, pltpu.roll(x, height - 1, 0), 0.0) - jnp.where(line > 0, pltpu.roll(x, 1, 0), 0.0)

    def columns_of(x):
        return jnp.where(lane < width - 1, pltpu.roll(x, width - 1, 1), 0.0) - jnp.where(lane > 0, pltpu.roll(x, 1, 1), 0.0)

    state, damping = [state_ref[f] for f in range(4)], [damping_ref[f] for f in range(4)]
    forcing, drag = forcing_of(state, damping, 0.5, rows_of, columns_of)
    drag = [x + SHIFT for x in drag]
    for f in range(4):
        basis_ref[0, f] = forcing[f]
    for c in range(GUESS):
        image = shifted([basis_ref[c, f] for f in range(4)], drag, 0.5 * dt_total, rows_of, columns_of)
        for f in range(4):
            basis_ref[c + 1, f] = image[f] * (1.0 / RADIUS)
    gram_out([lambda j=j: [basis_ref[j, f] for f in range(4)] for j in range(GUESS + 1)], table_ref, send_ref)


dot = functools.partial(jnp.dot, precision=HIGH, preferred_element_type=jnp.float32)
TILE = (SLOTS, LANES)


def tall(x):
    return jnp.concatenate([x, jnp.zeros((LANES - x.shape[0], LANES), jnp.float32)], axis=0)


def down_sum(x):
    return jnp.sum(x, axis=0, keepdims=True)


def across_sum(x):
    return jnp.sum(x, axis=1, keepdims=True)


def gram_matrix(received_ref, count):
    devices = received_ref.shape[0]
    tile = (-(-count // 8) * 8, LANES)
    row, lane = iota(tile, 0), iota(tile, 1)
    below = [jnp.zeros(tile, jnp.float32)] * 2
    for g in range(0, count, GROUP):
        at = g // GROUP * 2
        tiles = [(received_ref[d : d + 8, at, :], received_ref[d : d + 8, at + 1, :]) for d in range(0, devices, 8)]
        for part, packed in enumerate(tree_sum(tiles)):
            packed = jnp.concatenate([packed] * (tile[0] // 8), axis=0)
            for j in range(g, min(g + GROUP, count)):
                turned = pltpu.roll(packed, LANES - (j - g) * SLOTS, 1) if j > g else packed
                below[part] = jnp.where((row == j) & (lane < SLOTS), turned, below[part])
    return [jnp.where(lane <= row, x, flip(x)) for x in below]


def flip(x):
    return jnp.transpose(tall(x))[: x.shape[0]]


def added(terms):
    while len(terms) > 1:
        terms = [terms[k] + terms[k + 1] for k in range(0, len(terms) - 1, 2)] + terms[len(terms) // 2 * 2 :]
    return terms[0]


def columns_of(matrix, count):
    return [jnp.broadcast_to(matrix[:, a : a + 1], matrix.shape) for a in range(count)]


def weighted(columns, x):
    return added([x[a : a + 1] * column for a, column in enumerate(columns)])


def gram_schmidt(gram, image_of, start, count):
    row = iota(gram[0].shape, 0)
    raw, raw_image, inverse = jnp.where(row == 0, start, 0.0), gram[0] * start, 1.0
    vectors, images, hess = [raw], [], []
    for c in range(count):
        moved = image_of(raw, c)
        products = [down_sum(image * moved) for image in images]
        own = down_sum(raw_image * moved) * (inverse * inverse)
        images.append(raw_image * inverse)
        rest = added([moved] + [-product * other for product, other in zip(products, vectors)])
        seen = added([jnp.where(row == k, product, 0.0) for k, product in enumerate(products)] + [jnp.zeros_like(moved)])
        raw = rest * inverse - own * vectors[-1]
        column = seen * inverse + jnp.where(row == c, own, 0.0)
        raw_image = weighted(gram[: c + 2], raw)
        square = jnp.maximum(down_sum(raw * raw_image), 0.0) + norm_eps
        inverse = lax.rsqrt(square)
        inverse = inverse * (1.5 - 0.5 * square * inverse * inverse)
        vectors.append(raw * inverse)
        hess.append(column + jnp.where(row == c + 1, square * inverse, 0.0))
    return vectors, hess


def by_lane(columns, first, matrix):
    lane = iota(matrix.shape, 1)
    for k, column in enumerate(columns):
        matrix = jnp.where(lane == first + k, column, matrix)
    return matrix


def refined_gram(vectors, gram, gram_low):
    row = iota(gram[0].shape, 0)
    zero = jnp.zeros_like(gram[0])
    turned = by_lane(vectors, 0, zero)
    parts = split(turned)
    image = (zero, zero)
    for j, (column, low) in enumerate(zip(gram, gram_low)):
        line = slice(j, j + 1)
        image = add_product(image, column, turned[line], [part[line] for part in parts])
        image = image[0], image[1] + low * turned[line]
    image_parts = split(image[0])
    result = zero
    for c, vector in enumerate(vectors):
        high, low = add_product((zero, zero), vector, image[0], image_parts)
        low = low + vector * image[1]
        high, low = tree_sum([(high[r : r + 8], low[r : r + 8]) for r in range(0, row.shape[0], 8)])
        result = jnp.where(row == c, (high + low)[0:1], result)
    return result


def guessed(received_ref):
    gram = columns_of(gram_matrix(received_ref, GUESS + 1)[0], GUESS + 1)
    beta = jnp.sqrt(gram[0][0:1] + norm_eps)

    def image_of(x, c):
        return RADIUS * pltpu.roll(x, 1, 0) + SHIFT * x

    return gram_schmidt(gram, image_of, 1.0 / beta, GUESS)[1], beta


def basis_columns(guess):
    row = iota(TILE, 0)
    more = jnp.zeros((SLOTS - guess[0].shape[0], LANES), jnp.float32)
    columns = []
    for c, column in enumerate(guess):
        length = jnp.maximum(column[c + 1 : c + 2], 0.5 * RADIUS)
        columns.append(jnp.where(row == c + 1, length, jnp.concatenate([column, more], axis=0)))
    c = GUESS - 1
    shift = 0.5 * (guess[c - 1][c - 1 : c] + guess[c][c : c + 1])
    length = jnp.maximum(0.5 * (guess[c - 1][c : c + 1] + guess[c][c + 1 : c + 2]), 0.5 * RADIUS)
    back = guess[c][c - 1 : c]
    for c in range(GUESS, KRYLOV):
        column = jnp.where(row == c, shift, jnp.where(row == c + 1, length, 0.0))
        columns.append(jnp.where(row == c - 1, back, column))
    return columns


def orthogonalize(received_ref, steps, scale):
    slots = KRYLOV + 1
    gram, gram_low = [columns_of(x, slots) for x in gram_matrix(received_ref, slots)]
    beta = jnp.sqrt(scale * scale * gram[0][0:1] + norm_eps)
    vectors, image = gram_schmidt(gram, lambda x, c: weighted(steps[: c + 1], x), scale / beta, KRYLOV)
    gram = columns_of(refined_gram(vectors, gram, gram_low), slots)
    again, hess = gram_schmidt(gram, lambda x, c: weighted(image[: c + 1], x), 1.0, KRYLOV)
    return [weighted(vectors[: c + 1], x) for c, x in enumerate(again)], hess, beta


def combine(weights, parts):
    total = None
    for i, part in parts:
        value = part()
        scale = jnp.concatenate([weights[i : i + 1]] * (value.shape[1] // LANES), axis=1)
        total = scale * value if total is None else total + scale * value
    return total


def block_parts(basis_ref, f):
    return [(j, lambda j=j: basis_ref[j, f]) for j in range(KRYLOV + 1)]


def last_kernel(received_ref, small_ref, basis_ref, small_out_ref, peak_ref):
    steps = columns_of(small_ref[0], KRYLOV)
    vectors, hess, beta = orthogonalize(received_ref, steps, small_ref[1, 0:1])
    zero = jnp.zeros(TILE, jnp.float32)
    small_out_ref[0] = by_lane(hess, 0, zero)
    small_out_ref[1] = jnp.broadcast_to(beta, TILE)
    small_out_ref[2] = by_lane(vectors, 0, zero)
    for f in range(4):
        peak = jnp.max(jnp.abs(combine(vectors[KRYLOV], block_parts(basis_ref, f))), axis=0, keepdims=True)
        for d in range(peak_ref.shape[0]):
            peak_ref[d, f : f + 1] = peak


def exp_kernel(weights_ref, small_ref, state_ref, basis_ref, combined_ref, highest_ref):
    hess, beta, vectors = flip(small_ref[0]), small_ref[1, 0:1, 0:1], small_ref[2]
    size = SUBSTEPS * SLOTS
    row, lane = iota((size, LANES), 0), iota((size, LANES), 1)
    row_in, lane_in = row % SLOTS, lane % SLOTS
    same = (row // SLOTS == lane // SLOTS) & (lane < size)
    lower = jnp.where((row_in < KRYLOV) & (lane < KRYLOV), jnp.concatenate([hess] * SUBSTEPS, axis=0), 0.0)
    wide = lower
    for k in range(1, SUBSTEPS):
        wide = jnp.where(lane // SLOTS == k, pltpu.roll(lower, k * SLOTS, 1), wide)
    fraction = ((row // SLOTS) + 1).astype(jnp.float32) * (1.0 / SUBSTEPS)
    scaled = jnp.where(same, wide * fraction, 0.0)
    scaled = scaled + jnp.where(same & (row_in == KRYLOV) & (lane_in == 0), 1.0, 0.0)
    scaled = scaled * (1.0 / 2.0**squarings)
    unit = jnp.where(row == lane, 1.0, 0.0)

    def times(a, b):
        return dot(a, tall(b))

    power = [unit, scaled, times(scaled, scaled)]
    power += [times(power[2], scaled), times(power[2], power[2])]

    def group(k, count):
        total = None
        for i in range(count):
            term = power[i] * (1.0 / math.factorial(k + i))
            total = term if total is None else total + term
        return total

    top = taylor_degree - 4
    result = group(top, 5)
    while top > 0:
        top -= 4
        result = times(result, power[4]) + group(top, 4)
    for _ in range(squarings):
        result = times(result, result)
    mixing = jnp.zeros((1, LANES), jnp.float32)
    highest = jnp.zeros((1, 1), jnp.float32)
    for k in range(SUBSTEPS):
        tau = (k + 1) / SUBSTEPS
        factor = dt_total * tau
        g = result[k * SLOTS + KRYLOV : k * SLOTS + KRYLOV + 1, :]
        g = pltpu.roll(g, LANES - k * SLOTS, 1) if k else g
        mixing = mixing + weights_ref[k] * factor * beta * g
        estimate = (factor * tau) * beta * hess[KRYLOV - 1 : KRYLOV, KRYLOV : KRYLOV + 1] * jnp.abs(g[:, KRYLOV - 1 : KRYLOV])
        highest = jnp.maximum(highest, estimate)
    mixing = jnp.where(lane[0:1] < KRYLOV, mixing, 0.0)
    share = jnp.broadcast_to(across_sum(vectors * mixing), TILE)
    for f in range(4):
        combined_ref[f] = state_ref[f] + combine(share, block_parts(basis_ref, f))
    highest_ref[...] = jnp.broadcast_to(highest, highest_ref.shape)


def finish_kernel(highest_ref, peaks_ref, error_ref):
    error_ref[...] = jnp.max(peaks_ref[...], axis=0) * highest_ref[0:1, 0:1]


def shards(state, damping, weights):
    fields, height, width = state.shape
    columns = width + LANES
    lines = lax.axis_size("sub") * lax.axis_size("gx")
    sides = lax.axis_size("gy")
    devices = lines * sides
    f32 = lambda *shape: jax.ShapeDtypeStruct(shape, jnp.float32)
    near = lambda *shape: pltpu.VMEM(shape, jnp.float32)

    def call(kernel, outs, *args, smem=(), far=(), scratch=()):
        space = lambda k: pltpu.SMEM if k in smem else pltpu.HBM if k in far else pltpu.VMEM
        specs = [pl.BlockSpec(memory_space=space(k)) for k in range(len(args))]
        args = [a if k in smem else pltpu.with_memory_space_constraint(a, space(k)) for k, a in enumerate(args)]
        return pl.pallas_call(
            kernel,
            out_shape=outs,
            in_specs=specs,
            out_specs=[VMEM] * len(outs),
            scratch_shapes=list(scratch),
            compiler_params=pltpu.CompilerParams(vmem_limit_bytes=16 * 2**20),
        )(*args)

    exchange = lambda x, axes: lax.all_to_all(x, axes, 0, 0)
    table = lambda count: near(-(-count * SLOTS // LANES) * LANES, LANES)
    sends = lambda count: near(devices, -(-count // GROUP) * 2, LANES)
    whole = near(fields, height, width)
    state, damping, *edges = call(
        edge_kernel,
        [whole, whole] + [near(height, LANES)] * (1 if sides == 2 else 2),
        state,
        damping,
        far=(0, 1),
        scratch=[pltpu.SemaphoreType.DMA((2,))],
    )
    if sides == 2:
        halos = [lax.ppermute(edges[0], "gy", [(0, 1), (1, 0)])]
    else:
        halos = [
            lax.ppermute(edges[0], "gy", [((i + 1) % sides, i) for i in range(sides)]),
            lax.ppermute(edges[1], "gy", [(i, (i + 1) % sides) for i in range(sides)]),
        ]
    (send,) = call(
        guess_kernel,
        [sends(GUESS + 1)],
        state,
        damping,
        scratch=[near(GUESS + 1, fields, height, width), table(GUESS + 1)],
    )
    guess = exchange(send, ALL)
    number = len(halos)
    stack = (8 * (width // LANES) + number) * HALO
    packs = call(
        functools.partial(pack_kernel, number),
        [near(stack, LANES)] * (1 if height == HALO else 2),
        state,
        damping,
        *halos,
    )
    up = lax.ppermute(packs[0], ROWS, [(i, (i + 1) % lines) for i in range(lines)])
    down = lax.ppermute(packs[-1], ROWS, [((i + 1) % lines, i) for i in range(lines)])
    tall_rows = height + 2 * HALO
    basis, small, send = call(
        functools.partial(first_kernel, number),
        [near(KRYLOV + 1, fields, height, width), near(2, *TILE), sends(KRYLOV + 1)],
        state,
        damping,
        *halos,
        up,
        down,
        guess,
        scratch=[
            near(KRYLOV + 1, fields, tall_rows, columns),
            near(fields, tall_rows, columns),
            table(KRYLOV + 1),
        ],
    )
    small, peaks = call(
        last_kernel,
        [near(3, *TILE), near(lines, fields, width)],
        exchange(send, ALL),
        small,
        basis,
    )
    combined, highest = call(
        exp_kernel,
        [f32(fields, height, width), near(8, LANES)],
        weights,
        small,
        state,
        basis,
        smem=(0,),
    )
    (column_error,) = call(finish_kernel, [f32(fields, width)], highest, exchange(peaks, ROWS))
    return combined, column_error


def solution(mesh):
    return jax.shard_map(
        shards,
        mesh=mesh,
        in_specs=(P(None, ROWS, "gy"), P(None, ROWS, "gy"), P()),
        out_specs=(P(None, ROWS, "gy"), P(None, "gy")),
        check_vma=False,
    )
```

```python
import functools
import math

import jax
import jax.numpy as jnp
from jax import lax
from jax.experimental import pallas as pl
from jax.experimental.pallas import tpu as pltpu
from jax.sharding import PartitionSpec as P


KRYLOV = 12
SUBSTEPS = 4
GUESS = 6
REACH = KRYLOV + 1
HALO = -(-REACH // 8) * 8
LANES = 128
SLOTS = 16
EDGE = 16

dt_total = 4.0
buoyancy_sq = 0.5
norm_eps = 1e-06
taylor_degree = 12
squarings = 8
SHIFT = -2.0
RADIUS = 4.0

ROWS = ("sub", "gx")
ALL = ("sub", "gx", "gy")
HIGH = lax.Precision.HIGHEST
VMEM = pl.BlockSpec(memory_space=pltpu.VMEM)


def iota(shape, dim):
    return lax.broadcasted_iota(jnp.int32, shape, dim)


def rise_rows(x):
    return pltpu.roll(x, x.shape[0] - 1, 0) - pltpu.roll(x, 1, 0)


def rise_columns(x):
    return pltpu.roll(x, x.shape[1] - 1, 1) - pltpu.roll(x, 1, 1)


def grid_mask(rows, columns, halo_rows):
    line, lane = iota((rows, columns), 0), iota((rows, columns), 1)
    place = lax.axis_index("sub") * lax.axis_size("gx") + lax.axis_index("gx")
    last = lax.axis_size("sub") * lax.axis_size("gx") - 1
    side = lax.axis_index("gy")
    first_line = jnp.where(place > 0, 0, halo_rows)
    end_line = jnp.where(place < last, rows, rows - halo_rows)
    body = columns - LANES
    right_end = jnp.where(side < lax.axis_size("gy") - 1, body + EDGE, body)
    left_start = jnp.where(side > 0, columns - EDGE, columns)
    inside = (line >= first_line) & (line < end_line) & ((lane < right_end) | (lane >= left_start))
    return jnp.where(inside, 1.0, 0.0)


def shifted(fields, drag, double, rows_of=rise_rows, columns_of=rise_columns):
    vx, vy, b, p = fields
    return (
        -double * rows_of(p) - drag[0] * vx,
        -double * columns_of(p) + dt_total * b - drag[1] * vy,
        (-buoyancy_sq * dt_total) * vy - drag[2] * b,
        -double * (rows_of(vx) + columns_of(vy)) - drag[3] * p,
    )


def forcing_of(state, damping, half, rows_of=rise_rows, columns_of=rise_columns):
    vx, vy, b, p = state
    linear = (
        -half * rows_of(p),
        -half * columns_of(p) + b,
        -buoyancy_sq * vy,
        -half * (rows_of(vx) + columns_of(vy)),
    )
    square = [damping[f] * state[f] * state[f] for f in range(4)]
    return [linear[f] - square[f] * state[f] for f in range(4)], [(3.0 * dt_total) * x for x in square]


def two_sum(a, b):
    total = a + b
    part = total - a
    return total, (a - (total - part)) + (b - part)


def pair_sum(one, two):
    total, error = two_sum(one[0], two[0])
    return total, one[1] + two[1] + error


def split(a):
    scaled = 4097.0 * a
    high = scaled - (scaled - a)
    return high, a - high


def add_product(total, a, b, b_parts):
    product = a * b
    a_high, a_low = split(a)
    error = ((a_high * b_parts[0] - product) + a_high * b_parts[1] + a_low * b_parts[0]) + a_low * b_parts[1]
    high, rest = two_sum(total[0], product)
    return high, total[1] + (rest + error)


def tree_sum(tiles):
    while len(tiles) > 1:
        tiles = [pair_sum(tiles[k], tiles[k + 1]) for k in range(0, len(tiles) - 1, 2)] + tiles[len(tiles) // 2 * 2 :]
    total = tiles[0]
    for shift in (4, 2, 1):
        total = pair_sum(total, (pltpu.roll(total[0], shift, 0), pltpu.roll(total[1], shift, 0)))
    return total


def pair_rows(one, two):
    total = None
    for f in range(4):
        prod = one[f] * two[f]
        part = None
        for r in range(0, prod.shape[0], 8):
            for c in range(0, prod.shape[1], LANES):
                tile = prod[r : r + 8, c : c + LANES]
                part = tile if part is None else part + tile
        total = part if total is None else total + part
    return jnp.sum(total, axis=0, keepdims=True)


GROUP = LANES // SLOTS


def gram_out(vectors, table_ref, send_ref):
    table_ref[...] = jnp.zeros_like(table_ref)
    for j in range(len(vectors)):
        for i in range(j + 1):
            table_ref[j * SLOTS + i : j * SLOTS + i + 1, :] = pair_rows(vectors[i](), vectors[j]())
    zero = jnp.zeros((8, LANES), jnp.float32)
    for g in range(table_ref.shape[0] // LANES):
        turned = jnp.transpose(table_ref[g * LANES : (g + 1) * LANES])
        high, low = tree_sum([(turned[r : r + 8], zero) for r in range(0, LANES, 8)])
        for d in range(send_ref.shape[0]):
            send_ref[d, 2 * g : 2 * g + 1] = high[0:1]
            send_ref[d, 2 * g + 1 : 2 * g + 2] = low[0:1]


def edge_kernel(far_state_ref, far_damping_ref, state_ref, damping_ref, *refs):
    edge_refs, semaphores = refs[:-1], refs[-1]
    copies = [
        pltpu.make_async_copy(far_state_ref, state_ref, semaphores.at[0]),
        pltpu.make_async_copy(far_damping_ref, damping_ref, semaphores.at[1]),
    ]
    for copy in copies:
        copy.start()
    for copy in copies:
        copy.wait()
    width = state_ref.shape[2]
    lane = iota((state_ref.shape[1], LANES), 1)

    def packed(pick):
        total = None
        for k in range(8):
            ref = state_ref if k < 4 else damping_ref
            head, tail = ref[k % 4, :, :LANES], ref[k % 4, :, width - LANES :]
            tile = pltpu.roll(pick(head, pltpu.roll(tail, EDGE, 1)), k * EDGE, 1) if k else pick(head, pltpu.roll(tail, EDGE, 1))
            total = tile if total is None else jnp.where(lane // EDGE == k, tile, total)
        return total

    if len(edge_refs) == 1:
        left = lax.axis_index("gy") == 0
        edge_refs[0][...] = packed(lambda head, tail: jnp.where(left, tail, head))
    else:
        edge_refs[0][...] = packed(lambda head, tail: head)
        edge_refs[1][...] = packed(lambda head, tail: tail)


def pack_kernel(count, state_ref, damping_ref, *refs):
    halo_refs, out_refs = refs[:count], refs[count:]
    height, width = state_ref.shape[1:]
    for out_ref, start in zip(out_refs, (height - REACH, 0)):
        lines = slice(start, start + REACH)
        at = 0
        for k in range(8):
            ref = state_ref if k < 4 else damping_ref
            for c in range(0, width, LANES):
                out_ref[at : at + REACH] = ref[k % 4, lines, c : c + LANES]
                at += REACH
        for halo_ref in halo_refs:
            out_ref[at : at + REACH] = halo_ref[lines]
            at += REACH
        if at < out_ref.shape[0]:
            out_ref[at:] = jnp.zeros((out_ref.shape[0] - at, LANES), jnp.float32)


def first_kernel(count, state_ref, damping_ref, *refs):
    halo_refs = refs[:count]
    up_ref, down_ref, guess_ref, inner_ref, small_ref, send_ref, basis_ref, drag_ref, table_ref = refs[count:]
    height, width = state_ref.shape[1:]
    rows, columns = height + 2 * HALO, width + LANES
    tiles = width // LANES
    mask = grid_mask(rows, columns, HALO)

    def side_tile(k, right, left):
        lane = iota(right.shape, 1)
        right = pltpu.roll(right, LANES - k * EDGE, 1) if k else right
        return jnp.where(lane < LANES // 2, right, pltpu.roll(left, LANES - (k + 1) * EDGE, 1) if k < 7 else left)

    def neighbour(ref, k, above):
        def piece(n):
            lines = ref[n * REACH : (n + 1) * REACH]
            blank = jnp.zeros((HALO - REACH, LANES), jnp.float32)
            return jnp.concatenate([blank, lines] if above else [lines, blank], axis=0)

        parts = [piece(k * tiles + t) for t in range(tiles)]
        ends = [piece(8 * tiles + c) for c in range(count)]
        return jnp.concatenate(parts + [side_tile(k, ends[0], ends[-1])], axis=1)

    def whole(k):
        ref = state_ref if k < 4 else damping_ref
        own = jnp.concatenate([ref[k % 4], side_tile(k, halo_refs[0][...], halo_refs[-1][...])], axis=1)
        joined = jnp.concatenate([neighbour(up_ref, k, True), own, neighbour(down_ref, k, False)], axis=0)
        return jnp.where(mask > 0, joined, 0.0)

    state = [whole(f) for f in range(4)]
    damping = [whole(4 + f) for f in range(4)]
    forcing, drag = forcing_of(state, damping, 0.5 * mask)
    guess, scale = guessed(guess_ref)
    steps = basis_columns(guess)
    small_ref[0] = by_lane(steps, 0, jnp.zeros(TILE, jnp.float32))
    small_ref[1] = jnp.broadcast_to(scale, TILE)
    wide = lambda x: jnp.concatenate([x] * (columns // LANES), axis=1)
    start = wide(1.0 / scale)
    for f in range(4):
        basis_ref[0, f] = forcing[f] * start
        drag_ref[f] = drag[f]
    double = (0.5 * dt_total) * mask
    for c, column in enumerate(steps):
        skip = (HALO - (KRYLOV - c)) // 8 * 8 if c else 0
        lines = slice(skip, rows - skip)
        entry = lambda i: wide(column[i : i + 1])
        shift, inverse = entry(c), wide(1.0 / column[c + 1 : c + 2])
        current = [basis_ref[c, f, lines] for f in range(4)]
        image = shifted(current, [drag_ref[f, lines] + shift for f in range(4)], double[lines])
        for f in range(4):
            value = image[f]
            for i in range(0 if c < GUESS else c - 1, c):
                value = value - entry(i) * basis_ref[i, f, lines]
            basis_ref[c + 1, f, lines] = value * inverse

    for j in range(KRYLOV + 1):
        for f in range(4):
            inner_ref[j, f] = basis_ref[j, f, HALO : rows - HALO, :width]
    gram_out([lambda j=j: [inner_ref[j, f] for f in range(4)] for j in range(KRYLOV + 1)], table_ref, send_ref)


def guess_kernel(state_ref, damping_ref, send_ref, basis_ref, table_ref):
    height, width = state_ref.shape[1:]
    line, lane = iota((height, width), 0), iota((height, width), 1)

    def rows_of(x):
        return jnp.where(line < height - 1, pltpu.roll(x, height - 1, 0), 0.0) - jnp.where(line > 0, pltpu.roll(x, 1, 0), 0.0)

    def columns_of(x):
        return jnp.where(lane < width - 1, pltpu.roll(x, width - 1, 1), 0.0) - jnp.where(lane > 0, pltpu.roll(x, 1, 1), 0.0)

    state, damping = [state_ref[f] for f in range(4)], [damping_ref[f] for f in range(4)]
    forcing, drag = forcing_of(state, damping, 0.5, rows_of, columns_of)
    drag = [x + SHIFT for x in drag]
    for f in range(4):
        basis_ref[0, f] = forcing[f]
    for c in range(GUESS):
        image = shifted([basis_ref[c, f] for f in range(4)], drag, 0.5 * dt_total, rows_of, columns_of)
        for f in range(4):
            basis_ref[c + 1, f] = image[f] * (1.0 / RADIUS)
    gram_out([lambda j=j: [basis_ref[j, f] for f in range(4)] for j in range(GUESS + 1)], table_ref, send_ref)


dot = functools.partial(jnp.dot, precision=HIGH, preferred_element_type=jnp.float32)
TILE = (SLOTS, LANES)


def tall(x):
    return jnp.concatenate([x, jnp.zeros((LANES - x.shape[0], LANES), jnp.float32)], axis=0)


def down_sum(x):
    return jnp.sum(x, axis=0, keepdims=True)


def across_sum(x):
    return jnp.sum(x, axis=1, keepdims=True)


def gram_matrix(received_ref, count):
    devices = received_ref.shape[0]
    tile = (-(-count // 8) * 8, LANES)
    row, lane = iota(tile, 0), iota(tile, 1)
    below = [jnp.zeros(tile, jnp.float32)] * 2
    for g in range(0, count, GROUP):
        at = g // GROUP * 2
        tiles = [(received_ref[d : d + 8, at, :], received_ref[d : d + 8, at + 1, :]) for d in range(0, devices, 8)]
        for part, packed in enumerate(tree_sum(tiles)):
            packed = jnp.concatenate([packed] * (tile[0] // 8), axis=0)
            for j in range(g, min(g + GROUP, count)):
                turned = pltpu.roll(packed, LANES - (j - g) * SLOTS, 1) if j > g else packed
                below[part] = jnp.where((row == j) & (lane < SLOTS), turned, below[part])
    return [jnp.where(lane <= row, x, flip(x)) for x in below]


def flip(x):
    return jnp.transpose(tall(x))[: x.shape[0]]


def added(terms):
    while len(terms) > 1:
        terms = [terms[k] + terms[k + 1] for k in range(0, len(terms) - 1, 2)] + terms[len(terms) // 2 * 2 :]
    return terms[0]


def columns_of(matrix, count):
    return [jnp.broadcast_to(matrix[:, a : a + 1], matrix.shape) for a in range(count)]


def weighted(columns, x):
    return added([x[a : a + 1] * column for a, column in enumerate(columns)])


def gram_schmidt(gram, image_of, start, count):
    row = iota(gram[0].shape, 0)
    raw, raw_image, inverse = jnp.where(row == 0, start, 0.0), gram[0] * start, 1.0
    vectors, images, hess = [raw], [], []
    for c in range(count):
        moved = image_of(raw, c)
        products = [down_sum(image * moved) for image in images]
        own = down_sum(raw_image * moved) * (inverse * inverse)
        images.append(raw_image * inverse)
        rest = added([moved] + [-product * other for product, other in zip(products, vectors)])
        seen = added([jnp.where(row == k, product, 0.0) for k, product in enumerate(products)] + [jnp.zeros_like(moved)])
        raw = rest * inverse - own * vectors[-1]
        column = seen * inverse + jnp.where(row == c, own, 0.0)
        raw_image = weighted(gram[: c + 2], raw)
        square = jnp.maximum(down_sum(raw * raw_image), 0.0) + norm_eps
        inverse = lax.rsqrt(square)
        inverse = inverse * (1.5 - 0.5 * square * inverse * inverse)
        vectors.append(raw * inverse)
        hess.append(column + jnp.where(row == c + 1, square * inverse, 0.0))
    return vectors, hess


def by_lane(columns, first, matrix):
    lane = iota(matrix.shape, 1)
    for k, column in enumerate(columns):
        matrix = jnp.where(lane == first + k, column, matrix)
    return matrix


def refined_gram(vectors, gram, gram_low):
    row = iota(gram[0].shape, 0)
    zero = jnp.zeros_like(gram[0])
    turned = by_lane(vectors, 0, zero)
    parts = split(turned)
    image = (zero, zero)
    for j, (column, low) in enumerate(zip(gram, gram_low)):
        line = slice(j, j + 1)
        image = add_product(image, column, turned[line], [part[line] for part in parts])
        image = image[0], image[1] + low * turned[line]
    image_parts = split(image[0])
    result = zero
    for c, vector in enumerate(vectors):
        high, low = add_product((zero, zero), vector, image[0], image_parts)
        low = low + vector * image[1]
        high, low = tree_sum([(high[r : r + 8], low[r : r + 8]) for r in range(0, row.shape[0], 8)])
        result = jnp.where(row == c, (high + low)[0:1], result)
    return result


def guessed(received_ref):
    gram = columns_of(gram_matrix(received_ref, GUESS + 1)[0], GUESS + 1)
    beta = jnp.sqrt(gram[0][0:1] + norm_eps)

    def image_of(x, c):
        return RADIUS * pltpu.roll(x, 1, 0) + SHIFT * x

    return gram_schmidt(gram, image_of, 1.0 / beta, GUESS)[1], beta


def basis_columns(guess):
    row = iota(TILE, 0)
    more = jnp.zeros((SLOTS - guess[0].shape[0], LANES), jnp.float32)
    columns, lengths, top = [], [], 0.0
    for c, column in enumerate(guess):
        top = jnp.maximum(column[c + 1 : c + 2], top)
        length = jnp.maximum(column[c + 1 : c + 2], 0.125 * top)
        lengths.append(length)
        columns.append(jnp.where(row == c + 1, length, jnp.concatenate([column, more], axis=0)))
    c = GUESS - 1
    shift = 0.5 * (guess[c - 1][c - 1 : c] + guess[c][c : c + 1])
    length = 0.5 * (lengths[c - 1] + lengths[c])
    back = guess[c][c - 1 : c]
    for c in range(GUESS, KRYLOV):
        column = jnp.where(row == c, shift, jnp.where(row == c + 1, length, 0.0))
        columns.append(jnp.where(row == c - 1, back, column))
    return columns


def orthogonalize(received_ref, steps, scale):
    slots = KRYLOV + 1
    gram, gram_low = [columns_of(x, slots) for x in gram_matrix(received_ref, slots)]
    beta = jnp.sqrt(scale * scale * gram[0][0:1] + norm_eps)
    vectors, image = gram_schmidt(gram, lambda x, c: weighted(steps[: c + 1], x), scale / beta, KRYLOV)
    gram = columns_of(refined_gram(vectors, gram, gram_low), slots)
    again, hess = gram_schmidt(gram, lambda x, c: weighted(image[: c + 1], x), 1.0, KRYLOV)
    return [weighted(vectors[: c + 1], x) for c, x in enumerate(again)], hess, beta


def combine(weights, parts):
    total = None
    for i, part in parts:
        value = part()
        scale = jnp.concatenate([weights[i : i + 1]] * (value.shape[1] // LANES), axis=1)
        total = scale * value if total is None else total + scale * value
    return total


def block_parts(basis_ref, f):
    return [(j, lambda j=j: basis_ref[j, f]) for j in range(KRYLOV + 1)]


def last_kernel(received_ref, small_ref, basis_ref, small_out_ref, peak_ref):
    steps = columns_of(small_ref[0], KRYLOV)
    vectors, hess, beta = orthogonalize(received_ref, steps, small_ref[1, 0:1])
    zero = jnp.zeros(TILE, jnp.float32)
    small_out_ref[0] = by_lane(hess, 0, zero)
    small_out_ref[1] = jnp.broadcast_to(beta, TILE)
    small_out_ref[2] = by_lane(vectors, 0, zero)
    for f in range(4):
        peak = jnp.max(jnp.abs(combine(vectors[KRYLOV], block_parts(basis_ref, f))), axis=0, keepdims=True)
        for d in range(peak_ref.shape[0]):
            peak_ref[d, f : f + 1] = peak


def exp_kernel(weights_ref, small_ref, state_ref, basis_ref, combined_ref, highest_ref):
    hess, beta, vectors = flip(small_ref[0]), small_ref[1, 0:1, 0:1], small_ref[2]
    size = SUBSTEPS * SLOTS
    row, lane = iota((size, LANES), 0), iota((size, LANES), 1)
    row_in, lane_in = row % SLOTS, lane % SLOTS
    same = (row // SLOTS == lane // SLOTS) & (lane < size)
    lower = jnp.where((row_in < KRYLOV) & (lane < KRYLOV), jnp.concatenate([hess] * SUBSTEPS, axis=0), 0.0)
    wide = lower
    for k in range(1, SUBSTEPS):
        wide = jnp.where(lane // SLOTS == k, pltpu.roll(lower, k * SLOTS, 1), wide)
    fraction = ((row // SLOTS) + 1).astype(jnp.float32) * (1.0 / SUBSTEPS)
    scaled = jnp.where(same, wide * fraction, 0.0)
    scaled = scaled + jnp.where(same & (row_in == KRYLOV) & (lane_in == 0), 1.0, 0.0)
    scaled = scaled * (1.0 / 2.0**squarings)
    unit = jnp.where(row == lane, 1.0, 0.0)

    def times(a, b):
        return dot(a, tall(b))

    power = [unit, scaled, times(scaled, scaled)]
    power += [times(power[2], scaled), times(power[2], power[2])]

    def group(k, count):
        total = None
        for i in range(count):
            term = power[i] * (1.0 / math.factorial(k + i))
            total = term if total is None else total + term
        return total

    top = taylor_degree - 4
    result = group(top, 5)
    while top > 0:
        top -= 4
        result = times(result, power[4]) + group(top, 4)
    for _ in range(squarings):
        result = times(result, result)
    mixing = jnp.zeros((1, LANES), jnp.float32)
    highest = jnp.zeros((1, 1), jnp.float32)
    for k in range(SUBSTEPS):
        tau = (k + 1) / SUBSTEPS
        factor = dt_total * tau
        g = result[k * SLOTS + KRYLOV : k * SLOTS + KRYLOV + 1, :]
        g = pltpu.roll(g, LANES - k * SLOTS, 1) if k else g
        mixing = mixing + weights_ref[k] * factor * beta * g
        estimate = (factor * tau) * beta * hess[KRYLOV - 1 : KRYLOV, KRYLOV : KRYLOV + 1] * jnp.abs(g[:, KRYLOV - 1 : KRYLOV])
        highest = jnp.maximum(highest, estimate)
    mixing = jnp.where(lane[0:1] < KRYLOV, mixing, 0.0)
    share = jnp.broadcast_to(across_sum(vectors * mixing), TILE)
    for f in range(4):
        combined_ref[f] = state_ref[f] + combine(share, block_parts(basis_ref, f))
    highest_ref[...] = jnp.broadcast_to(highest, highest_ref.shape)


def finish_kernel(highest_ref, peaks_ref, error_ref):
    error_ref[...] = jnp.max(peaks_ref[...], axis=0) * highest_ref[0:1, 0:1]


def shards(state, damping, weights):
    fields, height, width = state.shape
    columns = width + LANES
    lines = lax.axis_size("sub") * lax.axis_size("gx")
    sides = lax.axis_size("gy")
    devices = lines * sides
    f32 = lambda *shape: jax.ShapeDtypeStruct(shape, jnp.float32)
    near = lambda *shape: pltpu.VMEM(shape, jnp.float32)

    def call(kernel, outs, *args, smem=(), far=(), scratch=()):
        space = lambda k: pltpu.SMEM if k in smem else pltpu.HBM if k in far else pltpu.VMEM
        specs = [pl.BlockSpec(memory_space=space(k)) for k in range(len(args))]
        args = [a if k in smem else pltpu.with_memory_space_constraint(a, space(k)) for k, a in enumerate(args)]
        return pl.pallas_call(
            kernel,
            out_shape=outs,
            in_specs=specs,
            out_specs=[VMEM] * len(outs),
            scratch_shapes=list(scratch),
            compiler_params=pltpu.CompilerParams(vmem_limit_bytes=16 * 2**20),
        )(*args)

    exchange = lambda x, axes: lax.all_to_all(x, axes, 0, 0)
    table = lambda count: near(-(-count * SLOTS // LANES) * LANES, LANES)
    sends = lambda count: near(devices, -(-count // GROUP) * 2, LANES)
    whole = near(fields, height, width)
    state, damping, *edges = call(
        edge_kernel,
        [whole, whole] + [near(height, LANES)] * (1 if sides == 2 else 2),
        state,
        damping,
        far=(0, 1),
        scratch=[pltpu.SemaphoreType.DMA((2,))],
    )
    (send,) = call(
        guess_kernel,
        [sends(GUESS + 1)],
        state,
        damping,
        scratch=[near(GUESS + 1, fields, height, width), table(GUESS + 1)],
    )
    guess = exchange(send, ALL)
    if sides == 2:
        halos = [lax.ppermute(edges[0], "gy", [(0, 1), (1, 0)])]
    else:
        halos = [
            lax.ppermute(edges[0], "gy", [((i + 1) % sides, i) for i in range(sides)]),
            lax.ppermute(edges[1], "gy", [(i, (i + 1) % sides) for i in range(sides)]),
        ]
    number = len(halos)
    stack = -(-(8 * (width // LANES) + number) * REACH // 8) * 8
    packs = call(
        functools.partial(pack_kernel, number),
        [near(stack, LANES)] * 2,
        state,
        damping,
        *halos,
    )
    up = lax.ppermute(packs[0], ROWS, [(i, (i + 1) % lines) for i in range(lines)])
    down = lax.ppermute(packs[-1], ROWS, [((i + 1) % lines, i) for i in range(lines)])
    tall_rows = height + 2 * HALO
    basis, small, send = call(
        functools.partial(first_kernel, number),
        [near(KRYLOV + 1, fields, height, width), near(2, *TILE), sends(KRYLOV + 1)],
        state,
        damping,
        *halos,
        up,
        down,
        guess,
        scratch=[
            near(KRYLOV + 1, fields, tall_rows, columns),
            near(fields, tall_rows, columns),
            table(KRYLOV + 1),
        ],
    )
    small, peaks = call(
        last_kernel,
        [near(3, *TILE), near(lines, fields, width)],
        exchange(send, ALL),
        small,
        basis,
    )
    combined, highest = call(
        exp_kernel,
        [f32(fields, height, width), near(8, LANES)],
        weights,
        small,
        state,
        basis,
        smem=(0,),
    )
    (column_error,) = call(finish_kernel, [f32(fields, width)], highest, exchange(peaks, ROWS))
    return combined, column_error


def solution(mesh):
    return jax.shard_map(
        shards,
        mesh=mesh,
        in_specs=(P(None, ROWS, "gy"), P(None, ROWS, "gy"), P()),
        out_specs=(P(None, ROWS, "gy"), P(None, "gy")),
        check_vma=False,
    )
```

```python
import functools
import math

import jax
import jax.numpy as jnp
from jax import lax
from jax.experimental import pallas as pl
from jax.experimental.pallas import tpu as pltpu
from jax.sharding import PartitionSpec as P


KRYLOV = 12
SUBSTEPS = 4
GUESS = 5
REACH = KRYLOV + 1
HALO = -(-REACH // 8) * 8
LANES = 128
SLOTS = 16
EDGE = 16

dt_total = 4.0
buoyancy_sq = 0.5
norm_eps = 1e-06
taylor_degree = 12
squarings = 8
SHIFT = -2.0
RADIUS = 4.0

ROWS = ("sub", "gx")
ALL = ("sub", "gx", "gy")
HIGH = lax.Precision.HIGHEST
VMEM = pl.BlockSpec(memory_space=pltpu.VMEM)


def iota(shape, dim):
    return lax.broadcasted_iota(jnp.int32, shape, dim)


def rise_rows(x):
    return pltpu.roll(x, x.shape[0] - 1, 0) - pltpu.roll(x, 1, 0)


def rise_columns(x):
    return pltpu.roll(x, x.shape[1] - 1, 1) - pltpu.roll(x, 1, 1)


def grid_mask(rows, columns, halo_rows):
    line, lane = iota((rows, columns), 0), iota((rows, columns), 1)
    place = lax.axis_index("sub") * lax.axis_size("gx") + lax.axis_index("gx")
    last = lax.axis_size("sub") * lax.axis_size("gx") - 1
    side = lax.axis_index("gy")
    first_line = jnp.where(place > 0, 0, halo_rows)
    end_line = jnp.where(place < last, rows, rows - halo_rows)
    body = columns - LANES
    right_end = jnp.where(side < lax.axis_size("gy") - 1, body + EDGE, body)
    left_start = jnp.where(side > 0, columns - EDGE, columns)
    inside = (line >= first_line) & (line < end_line) & ((lane < right_end) | (lane >= left_start))
    return jnp.where(inside, 1.0, 0.0)


def shifted(fields, drag, double, rows_of=rise_rows, columns_of=rise_columns):
    vx, vy, b, p = fields
    return (
        -double * rows_of(p) - drag[0] * vx,
        -double * columns_of(p) + dt_total * b - drag[1] * vy,
        (-buoyancy_sq * dt_total) * vy - drag[2] * b,
        -double * (rows_of(vx) + columns_of(vy)) - drag[3] * p,
    )


def forcing_of(state, damping, half, rows_of=rise_rows, columns_of=rise_columns):
    vx, vy, b, p = state
    linear = (
        -half * rows_of(p),
        -half * columns_of(p) + b,
        -buoyancy_sq * vy,
        -half * (rows_of(vx) + columns_of(vy)),
    )
    square = [damping[f] * state[f] * state[f] for f in range(4)]
    return [linear[f] - square[f] * state[f] for f in range(4)], [(3.0 * dt_total) * x for x in square]


def two_sum(a, b):
    total = a + b
    part = total - a
    return total, (a - (total - part)) + (b - part)


def pair_sum(one, two):
    total, error = two_sum(one[0], two[0])
    return total, one[1] + two[1] + error


def split(a):
    scaled = 4097.0 * a
    high = scaled - (scaled - a)
    return high, a - high


def add_product(total, a, b, b_parts):
    product = a * b
    a_high, a_low = split(a)
    error = ((a_high * b_parts[0] - product) + a_high * b_parts[1] + a_low * b_parts[0]) + a_low * b_parts[1]
    high, rest = two_sum(total[0], product)
    return high, total[1] + (rest + error)


def tree_sum(tiles):
    while len(tiles) > 1:
        tiles = [pair_sum(tiles[k], tiles[k + 1]) for k in range(0, len(tiles) - 1, 2)] + tiles[len(tiles) // 2 * 2 :]
    total = tiles[0]
    for shift in (4, 2, 1):
        total = pair_sum(total, (pltpu.roll(total[0], shift, 0), pltpu.roll(total[1], shift, 0)))
    return total


def pair_rows(one, two):
    total = None
    for f in range(4):
        prod = one[f] * two[f]
        part = None
        for r in range(0, prod.shape[0], 8):
            for c in range(0, prod.shape[1], LANES):
                tile = prod[r : r + 8, c : c + LANES]
                part = tile if part is None else part + tile
        total = part if total is None else total + part
    return jnp.sum(total, axis=0, keepdims=True)


GROUP = LANES // SLOTS


def gram_out(vectors, table_ref, send_ref):
    table_ref[...] = jnp.zeros_like(table_ref)
    for j in range(len(vectors)):
        for i in range(j + 1):
            table_ref[j * SLOTS + i : j * SLOTS + i + 1, :] = pair_rows(vectors[i](), vectors[j]())
    zero = jnp.zeros((8, LANES), jnp.float32)
    for g in range(table_ref.shape[0] // LANES):
        turned = jnp.transpose(table_ref[g * LANES : (g + 1) * LANES])
        high, low = tree_sum([(turned[r : r + 8], zero) for r in range(0, LANES, 8)])
        for d in range(send_ref.shape[0]):
            send_ref[d, 2 * g : 2 * g + 1] = high[0:1]
            send_ref[d, 2 * g + 1 : 2 * g + 2] = low[0:1]


def edge_kernel(far_state_ref, far_damping_ref, state_ref, damping_ref, *refs):
    edge_refs, semaphores = refs[:-1], refs[-1]
    copies = [
        pltpu.make_async_copy(far_state_ref, state_ref, semaphores.at[0]),
        pltpu.make_async_copy(far_damping_ref, damping_ref, semaphores.at[1]),
    ]
    for copy in copies:
        copy.start()
    for copy in copies:
        copy.wait()
    width = state_ref.shape[2]
    lane = iota((state_ref.shape[1], LANES), 1)

    def packed(pick):
        total = None
        for k in range(8):
            ref = state_ref if k < 4 else damping_ref
            head, tail = ref[k % 4, :, :LANES], ref[k % 4, :, width - LANES :]
            tile = pltpu.roll(pick(head, pltpu.roll(tail, EDGE, 1)), k * EDGE, 1) if k else pick(head, pltpu.roll(tail, EDGE, 1))
            total = tile if total is None else jnp.where(lane // EDGE == k, tile, total)
        return total

    if len(edge_refs) == 1:
        left = lax.axis_index("gy") == 0
        edge_refs[0][...] = packed(lambda head, tail: jnp.where(left, tail, head))
    else:
        edge_refs[0][...] = packed(lambda head, tail: head)
        edge_refs[1][...] = packed(lambda head, tail: tail)


def pack_kernel(count, state_ref, damping_ref, *refs):
    halo_refs, out_refs = refs[:count], refs[count:]
    height, width = state_ref.shape[1:]
    for out_ref, start in zip(out_refs, (height - REACH, 0)):
        lines = slice(start, start + REACH)
        at = 0
        for k in range(8):
            ref = state_ref if k < 4 else damping_ref
            for c in range(0, width, LANES):
                out_ref[at : at + REACH] = ref[k % 4, lines, c : c + LANES]
                at += REACH
        for halo_ref in halo_refs:
            out_ref[at : at + REACH] = halo_ref[lines]
            at += REACH
        if at < out_ref.shape[0]:
            out_ref[at:] = jnp.zeros((out_ref.shape[0] - at, LANES), jnp.float32)


def first_kernel(count, state_ref, damping_ref, *refs):
    halo_refs = refs[:count]
    up_ref, down_ref, small_ref, inner_ref, send_ref, basis_ref, drag_ref, table_ref = refs[count:]
    height, width = state_ref.shape[1:]
    rows, columns = height + 2 * HALO, width + LANES
    tiles = width // LANES
    mask = grid_mask(rows, columns, HALO)

    def side_tile(k, right, left):
        lane = iota(right.shape, 1)
        right = pltpu.roll(right, LANES - k * EDGE, 1) if k else right
        return jnp.where(lane < LANES // 2, right, pltpu.roll(left, LANES - (k + 1) * EDGE, 1) if k < 7 else left)

    def neighbour(ref, k, above):
        def piece(n):
            lines = ref[n * REACH : (n + 1) * REACH]
            blank = jnp.zeros((HALO - REACH, LANES), jnp.float32)
            return jnp.concatenate([blank, lines] if above else [lines, blank], axis=0)

        parts = [piece(k * tiles + t) for t in range(tiles)]
        ends = [piece(8 * tiles + c) for c in range(count)]
        return jnp.concatenate(parts + [side_tile(k, ends[0], ends[-1])], axis=1)

    def whole(k):
        ref = state_ref if k < 4 else damping_ref
        own = jnp.concatenate([ref[k % 4], side_tile(k, halo_refs[0][...], halo_refs[-1][...])], axis=1)
        joined = jnp.concatenate([neighbour(up_ref, k, True), own, neighbour(down_ref, k, False)], axis=0)
        return jnp.where(mask > 0, joined, 0.0)

    state = [whole(f) for f in range(4)]
    damping = [whole(4 + f) for f in range(4)]
    forcing, drag = forcing_of(state, damping, 0.5 * mask)
    steps, scale = columns_of(small_ref[0], KRYLOV), small_ref[1, 0:1]
    wide = lambda x: jnp.concatenate([x] * (columns // LANES), axis=1)
    start = wide(1.0 / scale)
    for f in range(4):
        basis_ref[0, f] = forcing[f] * start
        drag_ref[f] = drag[f]
    double = (0.5 * dt_total) * mask
    for c, column in enumerate(steps):
        skip = (HALO - (KRYLOV - c)) // 8 * 8 if c else 0
        lines = slice(skip, rows - skip)
        entry = lambda i: wide(column[i : i + 1])
        shift, inverse = entry(c), wide(1.0 / column[c + 1 : c + 2])
        current = [basis_ref[c, f, lines] for f in range(4)]
        image = shifted(current, [drag_ref[f, lines] + shift for f in range(4)], double[lines])
        for f in range(4):
            value = image[f]
            for i in range(0 if c < GUESS else c - 1, c):
                value = value - entry(i) * basis_ref[i, f, lines]
            basis_ref[c + 1, f, lines] = value * inverse

    for j in range(KRYLOV + 1):
        for f in range(4):
            inner_ref[j, f] = basis_ref[j, f, HALO : rows - HALO, :width]
    gram_out([lambda j=j: [inner_ref[j, f] for f in range(4)] for j in range(KRYLOV + 1)], table_ref, send_ref)


def guess_kernel(state_ref, damping_ref, send_ref, basis_ref, table_ref):
    height, width = state_ref.shape[1:]
    line, lane = iota((height, width), 0), iota((height, width), 1)

    def rows_of(x):
        return jnp.where(line < height - 1, pltpu.roll(x, height - 1, 0), 0.0) - jnp.where(line > 0, pltpu.roll(x, 1, 0), 0.0)

    def columns_of(x):
        return jnp.where(lane < width - 1, pltpu.roll(x, width - 1, 1), 0.0) - jnp.where(lane > 0, pltpu.roll(x, 1, 1), 0.0)

    state, damping = [state_ref[f] for f in range(4)], [damping_ref[f] for f in range(4)]
    forcing, drag = forcing_of(state, damping, 0.5, rows_of, columns_of)
    drag = [x + SHIFT for x in drag]
    for f in range(4):
        basis_ref[0, f] = forcing[f]
    for c in range(GUESS):
        image = shifted([basis_ref[c, f] for f in range(4)], drag, 0.5 * dt_total, rows_of, columns_of)
        for f in range(4):
            basis_ref[c + 1, f] = image[f] * (1.0 / RADIUS)
    gram_out([lambda j=j: [basis_ref[j, f] for f in range(4)] for j in range(GUESS + 1)], table_ref, send_ref)


dot = functools.partial(jnp.dot, precision=HIGH, preferred_element_type=jnp.float32)
TILE = (SLOTS, LANES)


def tall(x):
    return jnp.concatenate([x, jnp.zeros((LANES - x.shape[0], LANES), jnp.float32)], axis=0)


def down_sum(x):
    return jnp.sum(x, axis=0, keepdims=True)


def across_sum(x):
    return jnp.sum(x, axis=1, keepdims=True)


def gram_matrix(received_ref, count):
    devices = received_ref.shape[0]
    tile = (-(-count // 8) * 8, LANES)
    row, lane = iota(tile, 0), iota(tile, 1)
    below = [jnp.zeros(tile, jnp.float32)] * 2
    for g in range(0, count, GROUP):
        at = g // GROUP * 2
        tiles = [(received_ref[d : d + 8, at, :], received_ref[d : d + 8, at + 1, :]) for d in range(0, devices, 8)]
        for part, packed in enumerate(tree_sum(tiles)):
            packed = jnp.concatenate([packed] * (tile[0] // 8), axis=0)
            for j in range(g, min(g + GROUP, count)):
                turned = pltpu.roll(packed, LANES - (j - g) * SLOTS, 1) if j > g else packed
                below[part] = jnp.where((row == j) & (lane < SLOTS), turned, below[part])
    return [jnp.where(lane <= row, x, flip(x)) for x in below]


def flip(x):
    return jnp.transpose(tall(x))[: x.shape[0]]


def added(terms):
    while len(terms) > 1:
        terms = [terms[k] + terms[k + 1] for k in range(0, len(terms) - 1, 2)] + terms[len(terms) // 2 * 2 :]
    return terms[0]


def columns_of(matrix, count):
    return [jnp.broadcast_to(matrix[:, a : a + 1], matrix.shape) for a in range(count)]


def weighted(columns, x):
    return added([x[a : a + 1] * column for a, column in enumerate(columns)])


def gram_schmidt(gram, image_of, start, count):
    row = iota(gram[0].shape, 0)
    raw, raw_image, inverse = jnp.where(row == 0, start, 0.0), gram[0] * start, 1.0
    vectors, images, hess = [raw], [], []
    for c in range(count):
        moved = image_of(raw, c)
        products = [down_sum(image * moved) for image in images]
        own = down_sum(raw_image * moved) * (inverse * inverse)
        images.append(raw_image * inverse)
        rest = added([moved] + [-product * other for product, other in zip(products, vectors)])
        seen = added([jnp.where(row == k, product, 0.0) for k, product in enumerate(products)] + [jnp.zeros_like(moved)])
        raw = rest * inverse - own * vectors[-1]
        column = seen * inverse + jnp.where(row == c, own, 0.0)
        raw_image = weighted(gram[: c + 2], raw)
        square = jnp.maximum(down_sum(raw * raw_image), 0.0) + norm_eps
        inverse = lax.rsqrt(square)
        inverse = inverse * (1.5 - 0.5 * square * inverse * inverse)
        vectors.append(raw * inverse)
        hess.append(column + jnp.where(row == c + 1, square * inverse, 0.0))
    return vectors, hess


def by_lane(columns, first, matrix):
    lane = iota(matrix.shape, 1)
    for k, column in enumerate(columns):
        matrix = jnp.where(lane == first + k, column, matrix)
    return matrix


def refined_gram(vectors, gram, gram_low):
    row = iota(gram[0].shape, 0)
    zero = jnp.zeros_like(gram[0])
    turned = by_lane(vectors, 0, zero)
    parts = split(turned)
    image = (zero, zero)
    for j, (column, low) in enumerate(zip(gram, gram_low)):
        line = slice(j, j + 1)
        image = add_product(image, column, turned[line], [part[line] for part in parts])
        image = image[0], image[1] + low * turned[line]
    image_parts = split(image[0])
    result = zero
    for c, vector in enumerate(vectors):
        high, low = add_product((zero, zero), vector, image[0], image_parts)
        low = low + vector * image[1]
        high, low = tree_sum([(high[r : r + 8], low[r : r + 8]) for r in range(0, row.shape[0], 8)])
        result = jnp.where(row == c, (high + low)[0:1], result)
    return result


def guessed(received_ref):
    gram = columns_of(gram_matrix(received_ref, GUESS + 1)[0], GUESS + 1)
    beta = jnp.sqrt(gram[0][0:1] + norm_eps)

    def image_of(x, c):
        return RADIUS * pltpu.roll(x, 1, 0) + SHIFT * x

    return gram_schmidt(gram, image_of, 1.0 / beta, GUESS)[1], beta


def basis_columns(guess):
    row = iota(TILE, 0)
    more = jnp.zeros((SLOTS - guess[0].shape[0], LANES), jnp.float32)
    columns, lengths, top = [], [], 0.0
    for c, column in enumerate(guess):
        top = jnp.maximum(column[c + 1 : c + 2], top)
        length = jnp.maximum(column[c + 1 : c + 2], 0.125 * top)
        lengths.append(length)
        columns.append(jnp.where(row == c + 1, length, jnp.concatenate([column, more], axis=0)))
    c = GUESS - 1
    shift = 0.5 * (guess[c - 1][c - 1 : c] + guess[c][c : c + 1])
    length = 0.5 * (lengths[c - 1] + lengths[c])
    back = guess[c][c - 1 : c]
    for c in range(GUESS, KRYLOV):
        column = jnp.where(row == c, shift, jnp.where(row == c + 1, length, 0.0))
        columns.append(jnp.where(row == c - 1, back, column))
    return columns


def plan_kernel(guess_ref, small_ref):
    guess, scale = guessed(guess_ref)
    small_ref[0] = by_lane(basis_columns(guess), 0, jnp.zeros(TILE, jnp.float32))
    small_ref[1] = jnp.broadcast_to(scale, TILE)


def orthogonalize(received_ref, steps, scale):
    slots = KRYLOV + 1
    gram, gram_low = [columns_of(x, slots) for x in gram_matrix(received_ref, slots)]
    beta = jnp.sqrt(scale * scale * gram[0][0:1] + norm_eps)
    vectors, image = gram_schmidt(gram, lambda x, c: weighted(steps[: c + 1], x), scale / beta, KRYLOV)
    gram = columns_of(refined_gram(vectors, gram, gram_low), slots)
    again, hess = gram_schmidt(gram, lambda x, c: weighted(image[: c + 1], x), 1.0, KRYLOV)
    return [weighted(vectors[: c + 1], x) for c, x in enumerate(again)], hess, beta


def combine(weights, parts):
    total = None
    for i, part in parts:
        value = part()
        scale = jnp.concatenate([weights[i : i + 1]] * (value.shape[1] // LANES), axis=1)
        total = scale * value if total is None else total + scale * value
    return total


def block_parts(basis_ref, f):
    return [(j, lambda j=j: basis_ref[j, f]) for j in range(KRYLOV + 1)]


def last_kernel(received_ref, small_ref, basis_ref, small_out_ref, peak_ref):
    steps = columns_of(small_ref[0], KRYLOV)
    vectors, hess, beta = orthogonalize(received_ref, steps, small_ref[1, 0:1])
    zero = jnp.zeros(TILE, jnp.float32)
    small_out_ref[0] = by_lane(hess, 0, zero)
    small_out_ref[1] = jnp.broadcast_to(beta, TILE)
    small_out_ref[2] = by_lane(vectors, 0, zero)
    for f in range(4):
        peak = jnp.max(jnp.abs(combine(vectors[KRYLOV], block_parts(basis_ref, f))), axis=0, keepdims=True)
        for d in range(peak_ref.shape[0]):
            peak_ref[d, f : f + 1] = peak


def exp_kernel(weights_ref, small_ref, state_ref, basis_ref, combined_ref, highest_ref):
    hess, beta, vectors = flip(small_ref[0]), small_ref[1, 0:1, 0:1], small_ref[2]
    size = SUBSTEPS * SLOTS
    row, lane = iota((size, LANES), 0), iota((size, LANES), 1)
    row_in, lane_in = row % SLOTS, lane % SLOTS
    same = (row // SLOTS == lane // SLOTS) & (lane < size)
    lower = jnp.where((row_in < KRYLOV) & (lane < KRYLOV), jnp.concatenate([hess] * SUBSTEPS, axis=0), 0.0)
    wide = lower
    for k in range(1, SUBSTEPS):
        wide = jnp.where(lane // SLOTS == k, pltpu.roll(lower, k * SLOTS, 1), wide)
    fraction = ((row // SLOTS) + 1).astype(jnp.float32) * (1.0 / SUBSTEPS)
    scaled = jnp.where(same, wide * fraction, 0.0)
    scaled = scaled + jnp.where(same & (row_in == KRYLOV) & (lane_in == 0), 1.0, 0.0)
    scaled = scaled * (1.0 / 2.0**squarings)
    unit = jnp.where(row == lane, 1.0, 0.0)

    def times(a, b):
        return dot(a, tall(b))

    power = [unit, scaled, times(scaled, scaled)]
    power += [times(power[2], scaled), times(power[2], power[2])]

    def group(k, count):
        total = None
        for i in range(count):
            term = power[i] * (1.0 / math.factorial(k + i))
            total = term if total is None else total + term
        return total

    top = taylor_degree - 4
    result = group(top, 5)
    while top > 0:
        top -= 4
        result = times(result, power[4]) + group(top, 4)
    for _ in range(squarings):
        result = times(result, result)
    mixing = jnp.zeros((1, LANES), jnp.float32)
    highest = jnp.zeros((1, 1), jnp.float32)
    for k in range(SUBSTEPS):
        tau = (k + 1) / SUBSTEPS
        factor = dt_total * tau
        g = result[k * SLOTS + KRYLOV : k * SLOTS + KRYLOV + 1, :]
        g = pltpu.roll(g, LANES - k * SLOTS, 1) if k else g
        mixing = mixing + weights_ref[k] * factor * beta * g
        estimate = (factor * tau) * beta * hess[KRYLOV - 1 : KRYLOV, KRYLOV : KRYLOV + 1] * jnp.abs(g[:, KRYLOV - 1 : KRYLOV])
        highest = jnp.maximum(highest, estimate)
    mixing = jnp.where(lane[0:1] < KRYLOV, mixing, 0.0)
    share = jnp.broadcast_to(across_sum(vectors * mixing), TILE)
    for f in range(4):
        combined_ref[f] = state_ref[f] + combine(share, block_parts(basis_ref, f))
    highest_ref[...] = jnp.broadcast_to(highest, highest_ref.shape)


def finish_kernel(highest_ref, peaks_ref, error_ref):
    error_ref[...] = jnp.max(peaks_ref[...], axis=0) * highest_ref[0:1, 0:1]


def shards(state, damping, weights):
    fields, height, width = state.shape
    columns = width + LANES
    lines = lax.axis_size("sub") * lax.axis_size("gx")
    sides = lax.axis_size("gy")
    devices = lines * sides
    f32 = lambda *shape: jax.ShapeDtypeStruct(shape, jnp.float32)
    near = lambda *shape: pltpu.VMEM(shape, jnp.float32)

    def call(kernel, outs, *args, smem=(), far=(), scratch=()):
        space = lambda k: pltpu.SMEM if k in smem else pltpu.HBM if k in far else pltpu.VMEM
        specs = [pl.BlockSpec(memory_space=space(k)) for k in range(len(args))]
        args = [a if k in smem else pltpu.with_memory_space_constraint(a, space(k)) for k, a in enumerate(args)]
        return pl.pallas_call(
            kernel,
            out_shape=outs,
            in_specs=specs,
            out_specs=[VMEM] * len(outs),
            scratch_shapes=list(scratch),
            compiler_params=pltpu.CompilerParams(vmem_limit_bytes=16 * 2**20),
        )(*args)

    exchange = lambda x, axes: lax.all_to_all(x, axes, 0, 0)
    table = lambda count: near(-(-count * SLOTS // LANES) * LANES, LANES)
    sends = lambda count: near(devices, -(-count // GROUP) * 2, LANES)
    whole = near(fields, height, width)
    state, damping, *edges = call(
        edge_kernel,
        [whole, whole] + [near(height, LANES)] * (1 if sides == 2 else 2),
        state,
        damping,
        far=(0, 1),
        scratch=[pltpu.SemaphoreType.DMA((2,))],
    )
    (send,) = call(
        guess_kernel,
        [sends(GUESS + 1)],
        state,
        damping,
        scratch=[near(GUESS + 1, fields, height, width), table(GUESS + 1)],
    )
    guess = exchange(send, ALL)
    if sides == 2:
        halos = [lax.ppermute(edges[0], "gy", [(0, 1), (1, 0)])]
    else:
        halos = [
            lax.ppermute(edges[0], "gy", [((i + 1) % sides, i) for i in range(sides)]),
            lax.ppermute(edges[1], "gy", [(i, (i + 1) % sides) for i in range(sides)]),
        ]
    number = len(halos)
    stack = -(-(8 * (width // LANES) + number) * REACH // 8) * 8
    packs = call(
        functools.partial(pack_kernel, number),
        [near(stack, LANES)] * 2,
        state,
        damping,
        *halos,
    )
    up = lax.ppermute(packs[0], ROWS, [(i, (i + 1) % lines) for i in range(lines)])
    down = lax.ppermute(packs[-1], ROWS, [((i + 1) % lines, i) for i in range(lines)])
    tall_rows = height + 2 * HALO
    (small,) = call(plan_kernel, [near(2, *TILE)], guess)
    basis, send = call(
        functools.partial(first_kernel, number),
        [near(KRYLOV + 1, fields, height, width), sends(KRYLOV + 1)],
        state,
        damping,
        *halos,
        up,
        down,
        small,
        scratch=[
            near(KRYLOV + 1, fields, tall_rows, columns),
            near(fields, tall_rows, columns),
            table(KRYLOV + 1),
        ],
    )
    small, peaks = call(
        last_kernel,
        [near(3, *TILE), near(lines, fields, width)],
        exchange(send, ALL),
        small,
        basis,
    )
    combined, highest = call(
        exp_kernel,
        [f32(fields, height, width), near(8, LANES)],
        weights,
        small,
        state,
        basis,
        smem=(0,),
    )
    (column_error,) = call(finish_kernel, [f32(fields, width)], highest, exchange(peaks, ROWS))
    return combined, column_error


def solution(mesh):
    return jax.shard_map(
        shards,
        mesh=mesh,
        in_specs=(P(None, ROWS, "gy"), P(None, ROWS, "gy"), P()),
        out_specs=(P(None, ROWS, "gy"), P(None, "gy")),
        check_vma=False,
    )
```
